32 devices in a mesh: dp: 4 (over z), expert: 4 (over y, x), tensor: 2 (over core).
Axes of the slice: x: 2, y: 2, z: 4, core: 2. Of those that a mesh axis runs over, the one named last changes fastest.
Arguments:
- tokens: bfloat16 [512, 6144], P('dp', 'tensor'), may hold values from -6 to 6
- out_grad: bfloat16 [512, 6144], P('dp', 'tensor'), may hold values from -6 to 6
- router_weight: bfloat16 [6144, 4], P('tensor'), may hold values from -0.078125 to 0.078125
- gate_weight: bfloat16 [4, 6144, 8192], P('expert', 'tensor', 'dp'), may hold values from -0.078125 to 0.078125
- up_weight: bfloat16 [4, 6144, 8192], P('expert', 'tensor', 'dp'), may hold values from -0.078125 to 0.078125
- down_weight: bfloat16 [4, 8192, 6144], P('expert', 'dp', 'tensor'), may hold values from -0.0625 to 0.0625
- expert_index: int32 [512, 2], P('dp'), may hold values from 0 to 3, as said below
- slot_index: int32 [512, 2], P('dp'), may hold values from 0 to 95, as said below
Outputs:
- tokens_grad: bfloat16 [512, 6144], P(('dp', 'expert'), 'tensor')
- router_grad: float32 [6144, 4], P('tensor')
- gate_grad: bfloat16 [4, 6144, 8192], P('expert', 'tensor', 'dp')
- up_grad: bfloat16 [4, 6144, 8192], P('expert', 'tensor', 'dp')
- down_grad: bfloat16 [4, 8192, 6144], P('expert', 'dp', 'tensor')
The draws below stay inside these ranges and needn't reach their ends.
Inputs may be any that keep to these rules, and one draw needn't show every extreme that they name: `expert_index`: each row names two different experts; in each aligned block of 128 rows no expert is named more than 96 times, and one expert is named exactly 96 times in every block. `slot_index`: entry k of a row is a slot of the expert in entry k of the same row of expert_index; within one aligned block of 128 rows the choices of one expert have distinct slots.
All inputs are finite; a program needn't handle non-finite values.
Results may differ from the reference program's by a relative error of at most 0.025.
Values may be sent and summed in bfloat16 or wider, within the bound.
A program may use at most 128 MiB of HBM per device.

```python
from functools import partial
import jax
import jax.numpy as jnp
from jax import lax

D = 6144
FF = 8192
EXPERTS = 4
TOK_DEV = 128
CAP = 96
TOKENS = 512
SLOTS = 384
N_TENSOR = 2


def routing_block(block_key, busiest):
    load_key, order_key, token_key, swap_key, slot_key = jax.random.split(block_key, 5)
    shares = jax.random.randint(load_key, (EXPERTS - 1,), 1, 4)
    rest_picks = 2 * TOK_DEV - CAP
    other_loads = rest_picks * shares // jnp.sum(shares)
    leftover = rest_picks - jnp.sum(other_loads)
    other_loads = other_loads.at[jnp.argmin(shares)].add(leftover)
    others = (busiest + 1 + jax.random.permutation(order_key, EXPERTS - 1)) % EXPERTS
    expert_order = jnp.concatenate([jnp.reshape(busiest, (1,)), others]).astype(jnp.int32)
    run_counts = jnp.concatenate([jnp.array([CAP], jnp.int32), other_loads.astype(jnp.int32)])
    run_ends = jnp.cumsum(run_counts)
    run_starts = run_ends - run_counts
    pick_ids = jnp.arange(2 * TOK_DEV, dtype=jnp.int32)
    pick_run = jnp.sum((pick_ids[:, None] >= run_ends[None, :]).astype(jnp.int32), axis=1)
    pick_expert = expert_order[pick_run]
    pick_offset = pick_ids - run_starts[pick_run]
    tables = jax.vmap(partial(jax.random.permutation, x=CAP))(jax.random.split(slot_key, EXPERTS))
    pick_slot = tables[pick_expert, pick_offset]
    token_order = jax.random.permutation(token_key, TOK_DEV)
    first_pick = token_order
    second_pick = token_order + TOK_DEV
    expert_pair = jnp.stack([pick_expert[first_pick], pick_expert[second_pick]], axis=1)
    slot_pair = jnp.stack([pick_slot[first_pick], pick_slot[second_pick]], axis=1)
    swap_pair = jax.random.randint(swap_key, (TOK_DEV, 1), 0, 2) == 1
    expert_pair = jnp.where(swap_pair, expert_pair[:, ::-1], expert_pair)
    slot_pair = jnp.where(swap_pair, slot_pair[:, ::-1], slot_pair)
    return (expert_pair, slot_pair)


def make_routes(key):
    base_key = jax.random.fold_in(key, 7)
    row_blocks = TOKENS // TOK_DEV
    busiest = jax.random.randint(jax.random.fold_in(base_key, 1), (), 0, EXPERTS).astype(jnp.int32)
    block_keys = jax.random.split(jax.random.fold_in(base_key, 2), row_blocks)
    expert_pair, slot_pair = jax.vmap(partial(routing_block, busiest=busiest))(block_keys)
    return (expert_pair.reshape(TOKENS, 2).astype(jnp.int32), slot_pair.reshape(TOKENS, 2).astype(jnp.int32))


def draw_expert_index(key, part):
    return make_routes(key)[0]


def draw_slot_index(key, part):
    return make_routes(key)[1]


def shard_levels(stream_key, dims, cuts, smallest, largest):
    loudness = 1.0
    for position, parts in cuts:
        heights = jax.random.uniform(jax.random.fold_in(jax.random.fold_in(stream_key, 6), position), (parts,), jnp.float32, smallest / len(cuts), largest / len(cuts))
        loudness = loudness * jnp.repeat(jnp.exp(heights), dims[position] // parts).reshape((-1,) + (1,) * (len(dims) - 1 - position))
    return loudness


def normal_values(stream_key, dims, scale, reach, pieces=(), kind=jnp.bfloat16):
    entries = scale * jax.random.normal(stream_key, dims, jnp.float32)
    if pieces:
        entries = entries * shard_levels(stream_key, dims, pieces, -0.22, 0.18)
    return jnp.clip(entries, -reach, reach).astype(kind)


def setup_inputs(seed: int = 0) -> dict:
    key_list = jax.random.split(jax.random.key(seed), 9)
    tokens = normal_values(key_list[0], (TOKENS, D), 1.0, 6.0, ((0, 4), (1, 2)))
    out_grad = normal_values(key_list[1], (TOKENS, D), 1.0, 6.0, ((0, 4), (1, 2)))
    router_weight = normal_values(key_list[2], (D, EXPERTS), D ** -0.5, 0.078125, ((0, 2),))
    gate_weight = normal_values(key_list[3], (EXPERTS, D, FF), D ** -0.5, 0.078125, ((0, 4), (1, 2), (2, 4)))
    up_weight = normal_values(key_list[4], (EXPERTS, D, FF), D ** -0.5, 0.078125, ((0, 4), (1, 2), (2, 4)))
    down_weight = normal_values(key_list[5], (EXPERTS, FF, D), FF ** -0.5, 0.0625, ((0, 4), (1, 4), (2, 2)))
    expert_index = draw_expert_index(jax.random.fold_in(key_list[8], 71), 0)
    slot_index = draw_slot_index(jax.random.fold_in(key_list[8], 71), 0)
    return dict(tokens=tokens, out_grad=out_grad, router_weight=router_weight, gate_weight=gate_weight, up_weight=up_weight, down_weight=down_weight, expert_index=expert_index, slot_index=slot_index)


highest = lax.Precision.HIGHEST


def block_sum(left_side, right_side):
    block_width = D // N_TENSOR
    running = jnp.zeros((left_side.shape[0], right_side.shape[1]), jnp.float32)
    for row_block in range(N_TENSOR):
        partial_value = jnp.dot(left_side[:, row_block * block_width:(row_block + 1) * block_width], right_side[row_block * block_width:(row_block + 1) * block_width], preferred_element_type=jnp.float32)
        partial_value = lax.optimization_barrier(partial_value.astype(jnp.bfloat16)).astype(jnp.float32)
        running = running + partial_value
    return running


def expert_backward(operands):
    slot_tokens, slot_grads, slot_prob, gate_w, up_w, down_w = operands
    gate_sum = block_sum(slot_tokens, gate_w)
    up_sum = block_sum(slot_tokens, up_w)
    grad_act = block_sum(slot_grads, down_w.T)
    gate_sigmoid = jax.nn.sigmoid(gate_sum)
    hidden = (gate_sum * gate_sigmoid * up_sum).astype(jnp.bfloat16)
    prob_grad = jnp.sum(hidden.astype(jnp.float32) * grad_act, axis=1)
    act_grad = slot_prob.astype(jnp.float32)[:, None] * grad_act
    grad_gate = (act_grad * up_sum * gate_sigmoid * (1.0 + gate_sum * (1.0 - gate_sigmoid))).astype(jnp.bfloat16)
    grad_up = (act_grad * gate_sum * gate_sigmoid).astype(jnp.bfloat16)
    scaled_grads = (slot_prob.astype(jnp.float32)[:, None] * slot_grads.astype(jnp.float32)).astype(jnp.bfloat16)
    down_grad = jnp.dot(hidden.T, scaled_grads, preferred_element_type=jnp.float32).astype(jnp.bfloat16)
    gate_grad = jnp.dot(slot_tokens.T, grad_gate, preferred_element_type=jnp.float32).astype(jnp.bfloat16)
    up_grad = jnp.dot(slot_tokens.T, grad_up, preferred_element_type=jnp.float32).astype(jnp.bfloat16)
    slot_dx = jnp.dot(grad_gate, gate_w.T, preferred_element_type=jnp.float32) + jnp.dot(grad_up, up_w.T, preferred_element_type=jnp.float32)
    return slot_dx, prob_grad, gate_grad, up_grad, down_grad


def reference(tokens, out_grad, router_weight, gate_weight, up_weight, down_weight, expert_index, slot_index):
    logits = jnp.dot(tokens, router_weight, preferred_element_type=jnp.float32)
    chosen = jnp.take_along_axis(logits, expert_index, axis=1)
    pick_prob = jnp.stack([jax.nn.sigmoid(chosen[:, 0] - chosen[:, 1]), jax.nn.sigmoid(chosen[:, 1] - chosen[:, 0])], axis=1)
    prob_low = pick_prob.astype(jnp.bfloat16)
    row_block = (jnp.arange(TOKENS, dtype=jnp.int32) // TOK_DEV).astype(jnp.int32)
    slot_place = ((expert_index * (TOKENS // TOK_DEV) + row_block[:, None]) * CAP + slot_index).astype(jnp.int32)
    flat_place = slot_place.reshape(-1)
    slot_tokens = jnp.zeros((EXPERTS * SLOTS, D), jnp.bfloat16).at[flat_place].set(jnp.repeat(tokens, 2, axis=0))
    slot_grads = jnp.zeros((EXPERTS * SLOTS, D), jnp.bfloat16).at[flat_place].set(jnp.repeat(out_grad, 2, axis=0))
    slot_prob = jnp.zeros((EXPERTS * SLOTS,), jnp.bfloat16).at[flat_place].set(prob_low.reshape(-1))
    slot_dx, prob_grad, gate_grad, up_grad, down_grad = lax.map(expert_backward, (slot_tokens.reshape(EXPERTS, SLOTS, D), slot_grads.reshape(EXPERTS, SLOTS, D), slot_prob.reshape(EXPERTS, SLOTS), gate_weight, up_weight, down_weight))
    pick_dx = slot_dx.reshape(EXPERTS * SLOTS, D)[slot_place]
    pick_grad = prob_grad.reshape(-1)[slot_place]
    mixed_grad = jnp.sum(pick_prob * pick_grad, axis=1, keepdims=True)
    weights = pick_prob * (pick_grad - mixed_grad)
    onehot = (expert_index[:, :, None] == jnp.arange(EXPERTS, dtype=jnp.int32)[None, None, :]).astype(jnp.float32)
    logit_grad = jnp.sum(onehot * weights[:, :, None], axis=1)
    tokens_grad = (jnp.sum(pick_dx, axis=1) + jnp.dot(logit_grad, router_weight.astype(jnp.float32).T, precision=highest)).astype(jnp.bfloat16)
    router_grad = jnp.dot(tokens.astype(jnp.float32).T, logit_grad, precision=highest)
    return tokens_grad, router_grad, gate_grad, up_grad, down_grad
```

```python
import functools

import jax
import jax.numpy as jnp
from jax import lax
from jax.experimental import pallas as pl
from jax.experimental.pallas import tpu as pltpu
from jax.sharding import PartitionSpec as P

CAP = 96
F32 = jnp.float32
BF16 = jnp.bfloat16
LANES = 128
MESH = pl.DeviceIdType.MESH
VMEM_LIMIT = 67_043_328


def dot_nn(a, b):
    return lax.dot_general(a, b, (((1,), (0,)), ((), ())), preferred_element_type=F32)


def dot_nt(a, b):
    return lax.dot_general(a, b, (((1,), (1,)), ((), ())), preferred_element_type=F32)


def dot_tn(a, b):
    return lax.dot_general(a, b, (((0,), (0,)), ((), ())), preferred_element_type=F32)


def sigmoid(x):
    return 1.0 / (1.0 + jnp.exp(-x))


def three_pieces(x):
    high = x.astype(BF16).astype(F32)
    rest = x - high
    middle = rest.astype(BF16).astype(F32)
    return high, middle, rest - middle


def split_count(width, most):
    for count in range(most, 0, -1):
        if width % (count * LANES) == 0:
            return count
    return 1


def layer_kernel(
    n_dp, n_exp, n_ten, f_chunks, w_chunks,
    tokens, out_grad, router, index, gate_w, up_w, down_w,
    hidden_out, gg_out, gu_out, st_out, sg_out, dx_out, rg_out,
    gw, uw, db, tok, gra, st, sg, own, peer, tdx, ax, ay, bsend, brecv, csend, crecv, acc,
    idx, rw, logit_own, logit_peer, prob, sel, selt, spb, dacc,
    dsend, dz, d1, dx1, d2, dx2, lgr, term,
    load_sem, in_sem, idx_ss, idx_rs, z_ss, z_rs, p_ss, p_rs, r_ss, r_rs,
    t_ss, t_rs, lg_ss, lg_rs, a_ss, a_rs, b_ss, b_rs, c_ss, c_rs, dz_ss, dz_rs, de_ss, de_rs, out_sem,
):
    d = lax.axis_index("dp")
    e = lax.axis_index("expert")
    t = lax.axis_index("tensor")
    quarter, width = tok.shape[2], tok.shape[3]
    rows = n_exp * quarter
    half = quarter // 2
    hidden_w = gw.shape[1]
    fc = hidden_w // f_chunks
    wc = width // w_chunks
    x_id, y_id, far = e ^ 1, e ^ 2, e ^ 3

    def at_dp(k):
        return (lax.rem(d + k, n_dp), e, t)

    def at_exp(which):
        return (d, which, t)

    def at_ten(k):
        return (d, e, lax.rem(t + k, n_ten))

    def block_from(k):
        return lax.rem(d - k + n_dp, n_dp)

    def remote(src, dst, ss, rs, device):
        return pltpu.make_async_remote_copy(
            src_ref=src, dst_ref=dst, send_sem=ss, recv_sem=rs, device_id=device, device_id_type=MESH
        )

    shifts = []
    for k in range(1, n_dp // 2 + 1):
        shifts.append(k)
        if n_dp - k != k:
            shifts.append(n_dp - k)

    idx_load = pltpu.make_async_copy(index, idx.at[d], load_sem.at[0])
    rw_load = pltpu.make_async_copy(router, rw, load_sem.at[1])
    gw_load = pltpu.make_async_copy(gate_w, gw, load_sem.at[2])
    uw_load = pltpu.make_async_copy(up_w, uw, load_sem.at[3])
    ins = (tokens, out_grad)
    bufs = (tok, gra)
    slots = (st, sg)
    in_load = [pltpu.make_async_copy(ins[a], bufs[a].at[d], in_sem.at[a]) for a in range(2)]
    down_load = [
        pltpu.make_async_copy(down_w.at[pl.ds(j * fc, fc)], db.at[j % 2], load_sem.at[4 + j])
        for j in range(f_chunks)
    ]
    idx_load.start()
    in_load[0].start()
    in_load[1].start()
    rw_load.start()

    barrier = pltpu.get_barrier_semaphore()
    others = [at_dp(k) for k in range(1, n_dp)] + [at_exp(x_id), at_exp(y_id)]
    others += [at_ten(k) for k in range(1, n_ten)]
    for device in others:
        pl.semaphore_signal(barrier, inc=1, device_id=device, device_id_type=MESH)
    pl.semaphore_wait(barrier, len(others))

    def idx_copy(k):
        return remote(idx.at[d], idx.at[d], idx_ss.at[k - 1], idx_rs.at[k - 1], at_dp(k))

    def idx_arrival(k):
        b = block_from(k)
        return remote(idx.at[b], idx.at[b], idx_ss.at[k - 1], idx_rs.at[k - 1], at_dp(k))

    def z_copy(a, k):
        return remote(
            ins[a].at[e], bufs[a].at[d, e], z_ss.at[a, k - 1], z_rs.at[a, k - 1], at_dp(k)
        )

    def z_arrival(a, k):
        b = block_from(k)
        return remote(
            bufs[a].at[b, e], bufs[a].at[b, e], z_ss.at[a, k - 1], z_rs.at[a, k - 1], at_dp(k)
        )

    def plane_copy(a, k, side, quarter_id):
        b = block_from(k)
        ref = bufs[a].at[b, quarter_id]
        return remote(
            ref, ref, p_ss.at[a, k - 1, side], p_rs.at[a, k - 1, side], at_exp((x_id, y_id)[side])
        )

    def relay_copy(a, k, side, quarter_id):
        b = block_from(k)
        ref = bufs[a].at[b, quarter_id, pl.ds((1 - side) * half, half)]
        return remote(
            ref, ref, r_ss.at[a, k - 1, side], r_rs.at[a, k - 1, side], at_exp((x_id, y_id)[side])
        )

    for k in shifts:
        z_copy(0, k).start()
    idx_load.wait()
    for k in shifts:
        idx_copy(k).start()
    for k in shifts:
        z_copy(1, k).start()
    gw_load.start()
    uw_load.start()
    for j in range(min(2, f_chunks)):
        down_load[j].start()

    order = [(a, k) for a in range(2) for k in shifts]
    n_order = len(order)

    def hop_plane(a, k):
        z_arrival(a, k).wait_recv()
        plane_copy(a, k, 0, e).start()
        plane_copy(a, k, 1, e).start()

    def hop_relay(a, k):
        plane_copy(a, k, 0, x_id).wait_recv()
        relay_copy(a, k, 1, x_id).start()
        plane_copy(a, k, 1, y_id).wait_recv()
        relay_copy(a, k, 0, y_id).start()

    def hop_last(a, k):
        relay_copy(a, k, 0, far).wait_recv()
        relay_copy(a, k, 1, far).wait_recv()

    def to_slots(a, block):
        base = pl.multiple_of(block * CAP, 16)
        lanes = width // split_count(width, 6)

        def body(i, carry):
            cols = pl.ds(pl.multiple_of(i * lanes, LANES), lanes)
            values = bufs[a][block, :, :, cols].reshape(rows, lanes)
            slots[a][pl.ds(base, CAP), cols] = dot_nn(sel[block, :CAP], values).astype(BF16)
            return carry

        lax.fori_loop(0, width // lanes, body, 0)

    def make_select(block):
        pos = lax.broadcasted_iota(jnp.int32, (LANES, rows), 0)
        first = (idx[block, 0:1] == e) & (idx[block, 2:3] == pos)
        second = (idx[block, 1:2] == e) & (idx[block, 3:4] == pos)
        hot = jnp.where(first | second, 1.0, 0.0).astype(F32)
        sel[block] = hot.astype(BF16)
        selt[block] = hot.T.astype(BF16)

    def part_matmul(which, j):
        weight = (gw, uw)[which]
        cols = pl.ds(j * fc, fc)
        tile = fc // split_count(fc, 2)

        def body(i, carry):
            sub = pl.ds(pl.multiple_of(j * fc + i * tile, LANES), tile)
            own[which, :, sub] = dot_nn(st[...], weight[:, sub]).astype(BF16)
            return carry

        lax.fori_loop(0, fc // tile, body, 0)
        send_part(which, j)

    def part_copy(which, j, k):
        cols = pl.ds(j * fc, fc)
        return remote(
            own.at[which, :, cols],
            peer.at[k - 1, which, :, cols],
            t_ss.at[k - 1, which, j],
            t_rs.at[k - 1, which, j],
            at_ten(k),
        )

    def send_part(which, j):
        for k in range(1, n_ten):
            part_copy(which, j, k).start()

    def logits_of(block):
        logit_own[block] = dot_nt(rw[...], tok[block].reshape(rows, width))

    def logit_copy(k):
        return remote(
            logit_own, logit_peer.at[k - 1], lg_ss.at[k - 1], lg_rs.at[k - 1], at_ten(k)
        )

    work = [functools.partial(part_matmul, w, j) for w in range(2) for j in range(f_chunks)]
    done_tokens = False
    made = set()
    spread = n_order + 2 - (len(shifts) + 1)

    def own_block(a):
        in_load[a].wait()
        to_slots(a, d)

    for step in range(n_order + 2):
        if step < n_order:
            hop_plane(*order[step])
        if step == 0:
            rw_load.wait()
            make_select(d)
            own_block(0)
            logits_of(d)
        if 0 <= step - 1 < n_order:
            hop_relay(*order[step - 1])
        if 0 <= step - 2 < n_order:
            a, k = order[step - 2]
            hop_last(a, k)
            block = block_from(k)
            if a == 0:
                idx_arrival(k).wait_recv()
                make_select(block)
                logits_of(block)
            to_slots(a, block)
            if a == 0 and k == shifts[-1]:
                done_tokens = True
                for m in range(1, n_ten):
                    logit_copy(m).start()
                gw_load.wait()
                uw_load.wait()
        if step == len(shifts) + 1:
            own_block(1)
        if done_tokens:
            left = n_order + 2 - step
            share = -(-len(work) // left)
            for piece in work[:share]:
                piece()
            work = work[share:]
    for piece in work:
        piece()

    for k in shifts:
        idx_copy(k).wait_send()
    for a, k in order:
        z_copy(a, k).wait_send()
        for side in range(2):
            plane_copy(a, k, side, e).wait_send()
            relay_copy(a, k, 1 - side, (x_id, y_id)[side]).wait_send()

    for m in range(1, n_ten):
        logit_copy(m).wait()
    choice = lax.broadcasted_iota(jnp.int32, (8, rows), 0)
    for r in range(n_dp):
        logits = logit_own[r]
        for m in range(1, n_ten):
            logits = logits + logit_peer[m - 1, r]
        chosen = [
            jnp.sum(jnp.where(choice == idx[r, k : k + 1], logits, 0.0), axis=0, keepdims=True)
            for k in range(2)
        ]
        p0 = sigmoid(chosen[0] - chosen[1])
        p1 = sigmoid(chosen[1] - chosen[0])
        prob[r, 0:1] = p0
        prob[r, 1:2] = p1
        pos = lax.broadcasted_iota(jnp.int32, (CAP, rows), 0)
        first = (idx[r, 0:1] == e) & (idx[r, 2:3] == pos)
        second = (idx[r, 1:2] == e) & (idx[r, 3:4] == pos)
        low0 = p0.astype(BF16).astype(F32)
        low1 = p1.astype(BF16).astype(F32)
        picked = jnp.where(first, low0, 0.0) + jnp.where(second, low1, 0.0)
        column = jnp.sum(picked, axis=1, keepdims=True)
        spb[pl.ds(r * CAP, CAP)] = jnp.broadcast_to(column, (CAP, LANES))
    dacc[...] = jnp.zeros_like(dacc)

    def mix(j):
        for which in range(3):
            for k in range(1, n_ten):
                part_copy(which, j, k).wait()
        per = fc // LANES

        def body(i, carry):
            r = i // per
            base = pl.ds(pl.multiple_of(r * CAP, 16), CAP)
            cols = pl.ds(pl.multiple_of(j * fc + (i - r * per) * LANES, LANES), LANES)
            total = []
            for which in range(3):
                value = own[which, base, cols].astype(F32)
                for k in range(1, n_ten):
                    value = value + peer[k - 1, which, base, cols].astype(F32)
                total.append(value)
            g, u, ga = total
            s = sigmoid(g)
            gs = g * s
            hid = (gs * u).astype(BF16)
            dacc[base] = dacc[base] + hid.astype(F32) * ga
            act = spb[base] * ga
            own[0, base, cols] = hid
            own[1, base, cols] = (act * u * s * (1.0 + g * (1.0 - s))).astype(BF16)
            own[2, base, cols] = (act * gs).astype(BF16)
            return carry

        lax.fori_loop(0, n_dp * per, body, 0)

    for j in range(f_chunks):
        down_load[j].wait()
        tile = fc // split_count(fc, 2)

        def body(i, carry, j=j, tile=tile):
            sub = pl.ds(pl.multiple_of(j * fc + i * tile, LANES), tile)
            rows_in = pl.ds(pl.multiple_of(i * tile, LANES), tile)
            own[2, :, sub] = dot_nt(sg[...], db[j % 2, rows_in]).astype(BF16)
            return carry

        lax.fori_loop(0, fc // tile, body, 0)
        if j + 2 < f_chunks:
            down_load[j + 2].start()
        send_part(2, j)
        if j >= 1:
            mix(j - 1)
    mix(f_chunks - 1)

    st_store = pltpu.make_async_copy(st, st_out, out_sem.at[3])
    st_store.start()
    own_store = [
        pltpu.make_async_copy(own.at[w], (hidden_out, gg_out, gu_out)[w], out_sem.at[w])
        for w in range(3)
    ]
    for copy in own_store:
        copy.start()

    for r in range(n_dp):
        column = jnp.sum(dacc[pl.ds(r * CAP, CAP)], axis=1, keepdims=True)
        pos = lax.broadcasted_iota(jnp.int32, (CAP, rows), 0)
        for k in range(2):
            hit = (idx[r, k : k + 1] == e) & (idx[r, 2 + k : 3 + k] == pos)
            dsend[pl.ds(2 * r + k, 1)] = jnp.sum(
                jnp.where(hit, column, 0.0), axis=0, keepdims=True
            )

    def dz_copy(k):
        return remote(dsend, dz.at[k - 1], dz_ss.at[k - 1], dz_rs.at[k - 1], at_dp(k))

    def de_copy(side):
        return remote(
            (d1, d2)[side], (dx1, dx2)[side], de_ss.at[side], de_rs.at[side],
            at_exp((x_id, y_id)[side]),
        )

    for k in shifts:
        dz_copy(k).start()

    def scale_grads():
        lanes = width // split_count(width, 6)

        def body(i, carry):
            cols = pl.ds(pl.multiple_of(i * lanes, LANES), lanes)
            for r in range(n_dp):
                base = pl.ds(r * CAP, CAP)
                sg[base, cols] = (spb[base][:, 0:1] * sg[base, cols].astype(F32)).astype(BF16)
            return carry

        lax.fori_loop(0, width // lanes, body, 0)

    def router_one():
        total = dsend[...]
        for k in shifts:
            dz_copy(k).wait()
        for k in shifts:
            total = total + dz[k - 1]
        d1[...] = total
        de_copy(0).start()

    def router_two():
        de_copy(0).wait()
        d2[...] = d1[...] + dx1[...]
        de_copy(1).start()

    def router_three():
        de_copy(1).wait()
        total = d2[...] + dx2[...]
        for r in range(n_dp):
            g0 = total[2 * r : 2 * r + 1]
            g1 = total[2 * r + 1 : 2 * r + 2]
            p0, p1 = prob[r, 0:1], prob[r, 1:2]
            mixed = p0 * g0 + p1 * g1
            w0, w1 = p0 * (g0 - mixed), p1 * (g1 - mixed)
            lg = jnp.where(choice == idx[r, 0:1], w0, 0.0) + jnp.where(
                choice == idx[r, 1:2], w1, 0.0
            )
            for i, piece in enumerate(three_pieces(lg)):
                lgr[r, pl.ds(8 * i, 8)] = piece
        lanes = width // split_count(width, 6)

        def body(i, carry):
            cols = pl.ds(pl.multiple_of(i * lanes, LANES), lanes)
            out = jnp.zeros((24, lanes), F32)
            for r in range(n_dp):
                values = tok[r, :, :, cols].reshape(rows, lanes)
                out = out + dot_nn(lgr[r].astype(BF16), values)
            term[0:8, cols] = out[0:8] + out[8:16] + out[16:24]
            return carry

        lax.fori_loop(0, width // lanes, body, 0)

    def dx_chunk(c):
        tile = wc // split_count(wc, 3)

        def body(i, carry):
            cols = pl.ds(pl.multiple_of(c * wc + i * tile, LANES), tile)
            part = dot_nt(own[1], gw[cols]) + dot_nt(own[2], uw[cols])
            part = part.astype(BF16)
            for r in range(n_dp):
                one = dot_nn(selt[r][:, :CAP], part[r * CAP : (r + 1) * CAP]).astype(BF16)
                tdx[r, :, :, cols] = one.reshape(n_exp, quarter, tile)
            return carry

        lax.fori_loop(0, wc // tile, body, 0)

    def a_copy(c, side, which):
        cols = pl.ds(c * wc, wc)
        quarter_id = ((x_id, far), (y_id, far))[side][which]
        return remote(
            tdx.at[:, quarter_id, pl.ds(side * half, half), cols],
            (ax, ay)[side].at[which, :, :, cols],
            a_ss.at[c, side, which],
            a_rs.at[c, side, which],
            at_exp((x_id, y_id)[side]),
        )

    def b_copy(c, side):
        cols = pl.ds(c * wc, wc)
        return remote(
            bsend.at[side, :, :, cols],
            brecv.at[side, :, :, cols],
            b_ss.at[c, side],
            b_rs.at[c, side],
            at_exp((y_id, x_id)[side]),
        )

    def c_copy(c, k):
        cols = pl.ds(c * wc, wc)
        return remote(
            csend.at[lax.rem(d + k, n_dp), :, cols],
            crecv.at[k - 1, :, cols],
            c_ss.at[c, k - 1],
            c_rs.at[c, k - 1],
            at_dp(k),
        )

    def start_a(c):
        for which in (1, 0):
            for side in range(2):
                a_copy(c, side, which).start()

    def relay_b(c):
        cols = pl.ds(c * wc, wc)
        for side in range(2):
            a_copy(c, side, 1).wait()
            mine = tdx[:, (y_id, x_id)[side], pl.ds(side * half, half), cols].astype(F32)
            got = (ax, ay)[side][1, :, :, cols].astype(F32)
            bsend[side, :, :, cols] = (mine + got).astype(BF16)
            b_copy(c, side).start()

    def cross_c(c):
        cols = pl.ds(c * wc, wc)
        for side in range(2):
            a_copy(c, side, 0).wait()
            b_copy(c, side).wait()
            part = pl.ds(side * half, half)
            total = tdx[:, e, part, cols].astype(F32)
            total = total + (ax, ay)[side][0, :, :, cols].astype(F32)
            total = total + brecv[side, :, :, cols].astype(F32)
            csend[:, part, cols] = total.astype(BF16)
        for k in shifts:
            c_copy(c, k).start()

    def finish(c):
        cols = pl.ds(c * wc, wc)
        total = csend[d, :, cols].astype(F32)
        for k in shifts:
            c_copy(c, k).wait()
        for k in shifts:
            total = total + crecv[k - 1, :, cols].astype(F32)
        acc[:, cols] = total

    small = [router_one, router_two, router_three]
    for c in range(w_chunks + 3):
        if c < w_chunks:
            dx_chunk(c)
            start_a(c)
        if 0 <= c - 1 < w_chunks:
            relay_b(c - 1)
        if 0 <= c - 2 < w_chunks:
            cross_c(c - 2)
        if c == 1:
            scale_grads()
            sg_store = pltpu.make_async_copy(sg, sg_out, out_sem.at[4])
            sg_store.start()
        elif small and c >= 2:
            small.pop(0)()
        if 0 <= c - 3 < w_chunks:
            finish(c - 3)
    for job in small:
        job()

    mine = lgr[d]
    weights = jnp.concatenate([rw[...]] * 3, axis=0)
    whole = dot_tn(mine.astype(BF16), weights)
    logit_term = whole.reshape(n_exp, quarter, width)
    tdx_rows = logit_term
    acc2 = tdx_rows
    term[8:8 + rows] = acc2.reshape(rows, width)
    pick = term[pl.ds(pl.multiple_of(8 + e * quarter, 8), quarter)]
    st_store.wait()
    csend[0] = (acc[...] + pick).astype(BF16)
    dx_store = pltpu.make_async_copy(csend.at[0], dx_out, out_sem.at[5])
    dx_store.start()
    rg_store = pltpu.make_async_copy(term.at[pl.ds(0, 8)], rg_out, out_sem.at[6])
    rg_store.start()
    for copy in own_store:
        copy.wait()
    sg_store.wait()
    dx_store.wait()
    rg_store.wait()


def run_kernel(n_dp, n_exp, n_ten, tokens, out_grad, router_weight, gate_w, up_w, down_w, index):
    rows, width = tokens.shape
    hidden_w = gate_w.shape[1]
    quarter = rows // n_exp
    half = quarter // 2
    slots = n_dp * CAP
    f_chunks = split_count(hidden_w, 4)
    w_chunks = split_count(width, 4)
    fc = hidden_w // f_chunks
    n_choice = router_weight.shape[1]
    router = jnp.pad(router_weight.T, ((0, 8 - n_choice), (0, 0)))
    shape = jax.ShapeDtypeStruct
    any_spec = pl.BlockSpec(memory_space=pl.ANY)
    dma = pltpu.SemaphoreType.DMA
    vmem = pltpu.VMEM
    d_rows = -(-2 * n_dp // 8) * 8
    z = n_dp - 1
    m = max(n_ten - 1, 1)
    scratch = [
        vmem((width, hidden_w), BF16),
        vmem((width, hidden_w), BF16),
        vmem((2, fc, width), BF16),
        vmem((n_dp, n_exp, quarter, width), BF16),
        vmem((n_dp, n_exp, quarter, width), BF16),
        vmem((slots, width), BF16),
        vmem((slots, width), BF16),
        vmem((3, slots, hidden_w), BF16),
        vmem((m, 3, slots, hidden_w), BF16),
        vmem((n_dp, n_exp, quarter, width), BF16),
        vmem((2, n_dp, half, width), BF16),
        vmem((2, n_dp, half, width), BF16),
        vmem((2, n_dp, half, width), BF16),
        vmem((2, n_dp, half, width), BF16),
        vmem((n_dp, quarter, width), BF16),
        vmem((z, quarter, width), BF16),
        vmem((quarter, width), F32),
        vmem((n_dp, 8, rows), jnp.int32),
        vmem((8, width), BF16),
        vmem((n_dp, 8, rows), F32),
        vmem((m, n_dp, 8, rows), F32),
        vmem((n_dp, 8, rows), F32),
        vmem((n_dp, LANES, rows), BF16),
        vmem((n_dp, rows, LANES), BF16),
        vmem((slots, LANES), F32),
        vmem((slots, LANES), F32),
        vmem((d_rows, rows), F32),
        vmem((z, d_rows, rows), F32),
        vmem((d_rows, rows), F32),
        vmem((d_rows, rows), F32),
        vmem((d_rows, rows), F32),
        vmem((d_rows, rows), F32),
        vmem((n_dp, 24, rows), F32),
        vmem((8 + rows, width), F32),
        dma((4 + f_chunks,)),
        dma((2,)),
        dma((z,)), dma((z,)),
        dma((2, z)), dma((2, z)),
        dma((2, z, 2)), dma((2, z, 2)),
        dma((2, z, 2)), dma((2, z, 2)),
        dma((m, 3, f_chunks)), dma((m, 3, f_chunks)),
        dma((m,)), dma((m,)),
        dma((w_chunks, 2, 2)), dma((w_chunks, 2, 2)),
        dma((w_chunks, 2)), dma((w_chunks, 2)),
        dma((w_chunks, z)), dma((w_chunks, z)),
        dma((z,)), dma((z,)),
        dma((2,)), dma((2,)),
        dma((7,)),
    ]
    flops = 2 * slots * width * hidden_w * 5
    return pl.pallas_call(
        functools.partial(layer_kernel, n_dp, n_exp, n_ten, f_chunks, w_chunks),
        out_shape=(
            shape((slots, hidden_w), BF16),
            shape((slots, hidden_w), BF16),
            shape((slots, hidden_w), BF16),
            shape((slots, width), BF16),
            shape((slots, width), BF16),
            shape((quarter, width), BF16),
            shape((8, width), F32),
        ),
        in_specs=[any_spec] * 7,
        out_specs=(any_spec,) * 7,
        scratch_shapes=scratch,
        compiler_params=pltpu.CompilerParams(
            collective_id=0, has_side_effects=True, vmem_limit_bytes=VMEM_LIMIT
        ),
        cost_estimate=pl.CostEstimate(
            flops=flops, bytes_accessed=6 * width * hidden_w, transcendentals=0
        ),
        name="layer",
    )(
        tokens.reshape(n_exp, quarter, width),
        out_grad.reshape(n_exp, quarter, width),
        router, index, gate_w, up_w, down_w,
    )


def build(n_dp, n_exp, n_ten):
    def shards(
        tokens, out_grad, router_weight, gate_weight, up_weight, down_weight, expert_index, slot_index
    ):
        n_choice = router_weight.shape[1]
        index = jnp.concatenate([expert_index, slot_index], axis=1).T
        index = jnp.pad(index, ((0, 4), (0, 0)))
        hidden, grad_gate, grad_up, slot_tokens, scaled, tokens_grad, router_t = run_kernel(
            n_dp, n_exp, n_ten, tokens, out_grad, router_weight,
            gate_weight[0], up_weight[0], down_weight[0], index,
        )
        gate_grad = dot_tn(slot_tokens, grad_gate).astype(BF16)
        up_grad = dot_tn(slot_tokens, grad_up).astype(BF16)
        down_grad = dot_tn(hidden, scaled).astype(BF16)
        router_grad = router_t[:n_choice].T
        return (tokens_grad, router_grad, gate_grad[None], up_grad[None], down_grad[None])

    return shards


def solution(mesh):
    in_specs = (
        P("dp", "tensor"),
        P("dp", "tensor"),
        P("tensor", None),
        P("expert", "tensor", "dp"),
        P("expert", "tensor", "dp"),
        P("expert", "dp", "tensor"),
        P("dp", None),
        P("dp", None),
    )
    out_specs = (
        P(("dp", "expert"), "tensor"),
        P("tensor", None),
        P("expert", "tensor", "dp"),
        P("expert", "tensor", "dp"),
        P("expert", "dp", "tensor"),
    )
    shards = build(mesh.shape["dp"], mesh.shape["expert"], mesh.shape["tensor"])
    return jax.shard_map(shards, mesh=mesh, in_specs=in_specs, out_specs=out_specs, check_vma=False)
```

```python
import functools

import jax
import jax.numpy as jnp
from jax import lax
from jax.experimental import pallas as pl
from jax.experimental.pallas import tpu as pltpu
from jax.sharding import PartitionSpec as P

CAP = 96
LAGS = (1, 2)
LEADS = (0.5, 1.5)
EARLY_EVENTS = 3
F32 = jnp.float32
BF16 = jnp.bfloat16
LANES = 128
MESH = pl.DeviceIdType.MESH
VMEM_LIMIT = 67_043_328


def dot_nn(a, b):
    return lax.dot_general(a, b, (((1,), (0,)), ((), ())), preferred_element_type=F32)


def dot_nt(a, b):
    return lax.dot_general(a, b, (((1,), (1,)), ((), ())), preferred_element_type=F32)


def dot_tn(a, b):
    return lax.dot_general(a, b, (((0,), (0,)), ((), ())), preferred_element_type=F32)


def sigmoid(x):
    return 1.0 / (1.0 + jnp.exp(-x))


def three_pieces(x):
    high = x.astype(BF16).astype(F32)
    rest = x - high
    middle = rest.astype(BF16).astype(F32)
    return high, middle, rest - middle


def split_count(width, most):
    for count in range(most, 0, -1):
        if width % (count * LANES) == 0:
            return count
    return 1


def spare_columns(width):
    return width // 12 if width % (12 * LANES) == 0 else 0


def layer_kernel(
    n_dp, n_exp, n_ten, f_chunks, w_chunks, splits, dg_chunks,
    tokens, out_grad, router, chosen_in, place_in, gate_w, up_w, down_w,
    gg_out, gu_out, st_out, dg_out, dx_out, rg_out,
    gw, uw, dw, tok, gra, st, sg, own, peer, ax, ay, bsend, brecv, csend, crecv, acc,
    pick, place, rw, logit_own, logit_peer, prob, sel, selt, spb, dacc,
    dsend, dz, d1, dx1, d2, dx2, lgr, term, rgt,
    load_sem, in_sem, idx_ss, idx_rs, z_ss, z_rs, p_ss, p_rs, r_ss, r_rs,
    t_ss, t_rs, lg_ss, lg_rs, a_ss, a_rs, b_ss, b_rs, c_ss, c_rs, dz_ss, dz_rs, de_ss, de_rs, out_sem, dg_sem,
):
    d = lax.axis_index("dp")
    e = lax.axis_index("expert")
    t = lax.axis_index("tensor")
    quarter, width = tok.shape[2], tok.shape[3]
    rows = n_exp * quarter
    half = quarter // 2
    n_choice = rw.shape[0]
    hidden_w = gw.shape[1]
    fc = hidden_w // f_chunks
    wc = width // w_chunks
    extra = spare_columns(width)
    piece = (width - extra) // splits
    n_pieces = splits + (1 if extra else 0)
    x_id, y_id, far = e ^ 1, e ^ 2, e ^ 3
    tdx = gra
    last = n_dp - 1
    f_tile = fc // split_count(fc, 2)

    def at_dp(k):
        return (lax.rem(d + k, n_dp), e, t)

    def at_exp(which):
        return (d, which, t)

    def at_ten(k):
        return (d, e, lax.rem(t + k, n_ten))

    def remote(src, dst, ss, rs, device):
        return pltpu.make_async_remote_copy(
            src_ref=src, dst_ref=dst, send_sem=ss, recv_sem=rs, device_id=device, device_id_type=MESH
        )

    short = jnp.minimum(d, last - d)
    blocks, from_left = [d], [None]
    for j in range(last):
        inner = j < 2 * short
        distance = jnp.where(inner, j // 2 + 1, j - short + 1)
        left = jnp.where(inner, 1 - j % 2, jnp.where(2 * d > last, 1, 0))
        blocks.append(d + distance * (1 - 2 * left))
        from_left.append(left)
    shifts = range(1, n_dp)

    ins = (tokens, out_grad)
    bufs = (tok, gra)
    slots = (st, sg)
    load = pltpu.make_async_copy
    idx_load = [
        load(chosen_in, pick.at[d], load_sem.at[0]),
        load(place_in, place.at[d], load_sem.at[1]),
    ]
    rw_load = load(router, rw, load_sem.at[2])
    gw_load = load(gate_w, gw, load_sem.at[3])
    uw_load = load(up_w, uw, load_sem.at[4])
    dw_load = load(down_w, dw, load_sem.at[5])
    in_load = [load(ins[a], bufs[a].at[d], in_sem.at[a]) for a in range(2)]
    for copy in idx_load:
        copy.start()
    in_load[0].start()
    rw_load.start()

    barrier = pltpu.get_barrier_semaphore()
    others = [at_dp(k) for k in shifts] + [at_exp(x_id), at_exp(y_id)]
    others += [at_ten(k) for k in range(1, n_ten)]
    for device in others:
        pl.semaphore_signal(barrier, inc=1, device_id=device, device_id_type=MESH)
    pl.semaphore_wait(barrier, len(others))

    def idx_copy(k, which):
        ref = (pick, place)[which].at[d]
        return remote(ref, ref, idx_ss.at[which, k - 1], idx_rs.at[which, d], at_dp(k))

    def idx_arrival(p, which):
        ref = (pick, place)[which].at[blocks[p]]
        return remote(ref, ref, idx_ss.at[which, 0], idx_rs.at[which, blocks[p]], at_dp(1))

    def line_part(ref, h):
        if h == splits:
            return ref.at[:, :, pl.ds(splits * piece, extra)]
        return ref.at[e, :, pl.ds(h * piece, piece)]

    def z_own(a, h, side):
        other = jnp.minimum(d + 1, last) if side == 0 else jnp.maximum(d - 1, 0)
        return remote(
            line_part(ins[a], h),
            line_part(bufs[a].at[d], h),
            z_ss.at[a, h, 0, side],
            z_rs.at[a, h, d],
            (other, e, t),
        )

    def z_hand(a, p, h):
        ref = line_part(bufs[a].at[blocks[p]], h)
        other = jnp.where(from_left[p] == 1, jnp.minimum(d + 1, last), jnp.maximum(d - 1, 0))
        return remote(ref, ref, z_ss.at[a, h, p, 0], z_rs.at[a, h, blocks[p]], (other, e, t))

    def z_goes_on(p):
        return jnp.where(from_left[p] == 1, d < last, d > 0)

    side_open = (d < last, d > 0)

    def send_own(a, h):
        for side in range(2):
            copy = z_own(a, h, side)

            @pl.when(side_open[side])
            def _(copy=copy):
                copy.start()

    def plane_copy(a, p, h, side, quarter_id):
        ref = bufs[a].at[blocks[p], quarter_id, :, pl.ds(h * piece, piece)]
        return remote(
            ref, ref, p_ss.at[a, p - 1, h, side], p_rs.at[a, p - 1, h, side],
            at_exp((x_id, y_id)[side]),
        )

    def relay_copy(a, p, h, side, quarter_id):
        ref = bufs[a].at[
            blocks[p], quarter_id, pl.ds((1 - side) * half, half), pl.ds(h * piece, piece)
        ]
        return remote(
            ref, ref, r_ss.at[a, p - 1, h, side], r_rs.at[a, p - 1, h, side],
            at_exp((x_id, y_id)[side]),
        )

    for h in range(n_pieces):
        send_own(0, h)
    for copy in idx_load:
        copy.wait()
    for k in shifts:
        for which in range(2):
            idx_copy(k, which).start()
    in_load[1].start()
    gw_load.start()
    uw_load.start()
    dw_load.start()

    def hop_line(a, p, h):
        hand = z_hand(a, p, h)
        hand.wait_recv()

        @pl.when(z_goes_on(p))
        def _():
            hand.start()

    def hop_plane(a, p, h):
        plane_copy(a, p, h, 0, e).start()
        plane_copy(a, p, h, 1, e).start()

    def hop_relay(a, p, h):
        plane_copy(a, p, h, 0, x_id).wait_recv()
        relay_copy(a, p, h, 1, x_id).start()
        plane_copy(a, p, h, 1, y_id).wait_recv()
        relay_copy(a, p, h, 0, y_id).start()

    def hop_last(a, p, h):
        relay_copy(a, p, h, 0, far).wait_recv()
        relay_copy(a, p, h, 1, far).wait_recv()

    def to_slots(a, p):
        lanes = width // split_count(width, 6)

        def body(i, carry):
            cols = pl.ds(pl.multiple_of(i * lanes, LANES), lanes)
            values = bufs[a][blocks[p], :, :, cols].reshape(rows, lanes)
            slots[a][pl.ds(p * CAP, CAP), cols] = dot_nn(sel[p, :CAP], values).astype(BF16)
            return carry

        lax.fori_loop(0, width // lanes, body, 0)

    def hits(p, k, count):
        pos = lax.broadcasted_iota(jnp.int32, (count, rows), 0)
        b = blocks[p]
        return (pick[b, k : k + 1] == e) & (place[b, k : k + 1] == pos)

    def make_select(p):
        hot = jnp.where(hits(p, 0, LANES) | hits(p, 1, LANES), 1.0, 0.0).astype(F32)
        sel[p] = hot.astype(BF16)
        selt[p] = hot.T.astype(BF16)

    def part_copy(which, j, k):
        cols = pl.ds(j * fc, fc)
        return remote(
            own.at[which, :, cols],
            peer.at[k - 1, which, :, cols],
            t_ss.at[k - 1, which, j],
            t_rs.at[k - 1, which, j],
            at_ten(k),
        )

    def part_tile(which, j, i):
        sub = pl.ds(pl.multiple_of(j * fc + i * f_tile, LANES), f_tile)
        if which < 2:
            value = dot_nn(st[...], (gw, uw)[which][:, sub])
        else:
            value = dot_nt(sg[...], dw[sub])
        own[which, :, sub] = value.astype(BF16)

    def send_part(which, j):
        for k in range(1, n_ten):
            part_copy(which, j, k).start()

    def part_matmul(which, j):
        def body(i, carry):
            part_tile(which, j, i)
            return carry

        lax.fori_loop(0, fc // f_tile, body, 0)
        send_part(which, j)

    def logits_of(p):
        logit_own[p] = dot_nt(rw[...], tok[blocks[p]].reshape(rows, width))

    def logit_copy(k):
        return remote(
            logit_own, logit_peer.at[k - 1], lg_ss.at[k - 1], lg_rs.at[k - 1], at_ten(k)
        )

    choice = lax.broadcasted_iota(jnp.int32, (n_choice, rows), 0)

    def routing():
        for m in range(1, n_ten):
            logit_copy(m).wait()
        for p in range(n_dp):
            logits = logit_own[p]
            for m in range(1, n_ten):
                logits = logits + logit_peer[m - 1, p]
            b = blocks[p]
            chosen = [
                jnp.sum(jnp.where(choice == pick[b, k : k + 1], logits, 0.0), axis=0, keepdims=True)
                for k in range(2)
            ]
            p0 = sigmoid(chosen[0] - chosen[1])
            p1 = sigmoid(chosen[1] - chosen[0])
            prob[p, 0:1] = p0
            prob[p, 1:2] = p1
            low0 = p0.astype(BF16).astype(F32)
            low1 = p1.astype(BF16).astype(F32)
            picked = jnp.where(hits(p, 0, CAP), low0, 0.0) + jnp.where(hits(p, 1, CAP), low1, 0.0)
            column = jnp.sum(picked, axis=1, keepdims=True)
            spb[pl.ds(p * CAP, CAP)] = jnp.broadcast_to(column, (CAP, LANES))
        dacc[...] = jnp.zeros_like(dacc)

    def mix_block(p, cols):
        base = pl.ds(p * CAP, CAP)
        total = []
        for which in range(3):
            value = own[which, base, cols].astype(F32)
            for k in range(1, n_ten):
                value = value + peer[k - 1, which, base, cols].astype(F32)
            total.append(value)
        g, u, ga = total
        s = sigmoid(g)
        gs = g * s
        hid = (gs * u).astype(BF16)
        dacc[base] = dacc[base] + hid.astype(F32) * ga
        act = spb[base] * ga
        own[0, base, cols] = hid
        own[1, base, cols] = (act * u * s * (1.0 + g * (1.0 - s))).astype(BF16)
        own[2, base, cols] = (act * gs).astype(BF16)

    def mix_wait(j):
        for which in range(3):
            for k in range(1, n_ten):
                part_copy(which, j, k).wait()

    def mix_tile(j, i):
        for q in range(f_tile // LANES):
            cols = pl.ds(pl.multiple_of(j * fc + i * f_tile + q * LANES, LANES), LANES)
            for p in range(n_dp):
                mix_block(p, cols)

    def mix(j):
        mix_wait(j)

        def body(i, carry):
            mix_tile(j, i)
            return carry

        lax.fori_loop(0, fc // f_tile, body, 0)

    pairs = [range(p, min(p + 2, n_dp)) for p in range(1, n_dp, 2)]
    orders = [[(a, p, h) for pair in pairs for h in range(splits) for p in pair] for a in range(2)]
    order = orders[0] + orders[1]
    beyond = [[(a, p, splits) for p in range(1, n_dp)] if extra else [] for a in range(2)]
    events = []
    for i, (a, p, h) in enumerate(order):
        lag = LAGS[a]
        ahead = LEADS[a] if i else 0
        events.append((i - ahead, 0, hop_line, (a, p, h)))
        events.append((i, 1, hop_plane, (a, p, h)))
        events.append((i + lag, 2, hop_relay, (a, p, h)))
        events.append((i + 2 * lag, 3, hop_last, (a, p, h)))
    for a in range(2):
        for i, which in enumerate(beyond[a]):
            time = len(orders[0]) * (a + 1) - len(beyond[a]) + i
            events.append((time + 0.5, 4, hop_line, which))
    events.sort(key=lambda event: event[:2])
    work = []
    left = [set(orders[a] + beyond[a]) for a in range(2)]
    events_left = len(events)
    tokens_done = False
    for position, (_, _, hop, which) in enumerate(events):
        hop(*which)
        events_left -= 1
        if position == EARLY_EVENTS:
            make_select(0)
            rw_load.wait()
            in_load[0].wait()
            to_slots(0, 0)
            logits_of(0)
        if hop is hop_line:
            if which == order[len(pairs[0]) - 1]:
                for h in range(n_pieces):
                    send_own(1, h)
        if hop is hop_last or which[2] == splits:
            a, p, h = which
            left[a].discard(which)
            if not any(other[1] == p for other in left[a]):
                if a == 0:
                    for kind in range(2):
                        idx_arrival(p, kind).wait_recv()
                    make_select(p)
                    logits_of(p)
                to_slots(a, p)
            if a == 0 and not left[0]:
                for m in range(1, n_ten):
                    logit_copy(m).start()
                in_load[1].wait()
                to_slots(1, 0)
                gw_load.wait()
                uw_load.wait()
                work += [functools.partial(part_matmul, w, j) for w in range(2) for j in range(f_chunks)]
                work.append(routing)
                tokens_done = True
        if tokens_done and work and hop in (hop_plane, hop_relay, hop_last):
            work.pop(0)()
    for job in work:
        job()
    dw_load.wait()

    for k in shifts:
        for which in range(2):
            idx_copy(k, which).wait_send()
    for a in range(2):
        for h in range(n_pieces):
            for side in range(2):
                copy = z_own(a, h, side)

                @pl.when(side_open[side])
                def _(copy=copy):
                    copy.wait_send()

    for a, p, h in order + beyond[0] + beyond[1]:
        hand = z_hand(a, p, h)

        @pl.when(z_goes_on(p))
        def _(hand=hand):
            hand.wait_send()

    for a, p, h in order:
        for side in range(2):
            plane_copy(a, p, h, side, e).wait_send()
            relay_copy(a, p, h, 1 - side, (x_id, y_id)[side]).wait_send()
    for j in range(f_chunks + 1):
        if j < f_chunks:
            part_matmul(2, j)
        if j >= 1:
            mix(j - 1)

    st_store = load(st, st_out, out_sem.at[3])
    st_store.start()
    own_store = [
        load(own.at[w], (None, gg_out, gu_out)[w], out_sem.at[w]) for w in (1, 2)
    ]
    for copy in own_store:
        copy.start()

    def router_zero():
        for p in range(n_dp):
            column = jnp.sum(dacc[pl.ds(p * CAP, CAP)], axis=1, keepdims=True)
            for k in range(2):
                dsend[blocks[p], k : k + 1] = jnp.sum(
                    jnp.where(hits(p, k, CAP), column, 0.0), axis=0, keepdims=True
                )
        for k in shifts:
            dz_copy(k).start()

    def dz_copy(k):
        return remote(dsend, dz.at[k - 1], dz_ss.at[k - 1], dz_rs.at[k - 1], at_dp(k))

    def de_copy(side):
        return remote(
            (d1, d2)[side], (dx1, dx2)[side], de_ss.at[side], de_rs.at[side],
            at_exp((x_id, y_id)[side]),
        )

    def scale_grads():
        lanes = width // split_count(width, 6)

        def body(i, carry):
            cols = pl.ds(pl.multiple_of(i * lanes, LANES), lanes)
            for p in range(n_dp):
                base = pl.ds(p * CAP, CAP)
                sg[base, cols] = (spb[base][:, 0:1] * sg[base, cols].astype(F32)).astype(BF16)
            return carry

        lax.fori_loop(0, width // lanes, body, 0)

    def router_one():
        total = dsend[...]
        for k in shifts:
            dz_copy(k).wait()
        for k in shifts:
            total = total + dz[k - 1]
        d1[...] = total
        de_copy(0).start()

    def router_two():
        de_copy(0).wait()
        d2[...] = d1[...] + dx1[...]
        de_copy(1).start()

    lanes = width // split_count(width, 6)

    def router_three():
        de_copy(1).wait()
        dx2[...] = d2[...] + dx2[...]
        for p in range(n_dp):
            b = blocks[p]
            g0, g1 = dx2[b, 0:1], dx2[b, 1:2]
            p0, p1 = prob[p, 0:1], prob[p, 1:2]
            mixed = p0 * g0 + p1 * g1
            w0, w1 = p0 * (g0 - mixed), p1 * (g1 - mixed)
            lg = jnp.where(choice == pick[b, 0:1], w0, 0.0) + jnp.where(
                choice == pick[b, 1:2], w1, 0.0
            )
            for i, part in enumerate(three_pieces(lg)):
                lgr[p, pl.ds(n_choice * i, n_choice)] = part
        weights = jnp.concatenate([rw[...].astype(F32)] * 3, axis=0).astype(BF16)

        def body(i, carry):
            cols = pl.ds(pl.multiple_of(i * lanes, LANES), lanes)
            out = jnp.zeros((3 * n_choice, lanes), F32)
            for p in range(n_dp):
                values = tok[blocks[p], :, :, cols].reshape(rows, lanes)
                out = out + dot_nn(lgr[p].astype(BF16), values)
            rgt[:, cols] = (
                out[0:n_choice] + out[n_choice : 2 * n_choice] + out[2 * n_choice : 3 * n_choice]
            )
            return carry

        lax.fori_loop(0, width // lanes, body, 0)
        term[...] = jnp.zeros_like(term)
        term[pl.ds(0, 3 * n_choice)] = lgr[0]
        term[...] = term[...].T
        mine = term[pl.ds(pl.multiple_of(e * quarter, 8), quarter)][:, : 3 * n_choice].astype(BF16)
        for i in range(width // lanes):
            cols = slice(i * lanes, (i + 1) * lanes)
            acc[:, cols] = dot_nn(mine, weights[:, cols])

    def dx_chunk(c):
        tile = wc // split_count(wc, 3)

        def body(i, carry):
            cols = pl.ds(pl.multiple_of(c * wc + i * tile, LANES), tile)
            part = dot_nt(own[1], gw[cols]) + dot_nt(own[2], uw[cols])
            part = part.astype(BF16)
            for p in range(n_dp):
                one = dot_nn(selt[p][:, :CAP], part[p * CAP : (p + 1) * CAP]).astype(BF16)
                tdx[p, :, :, cols] = one.reshape(n_exp, quarter, tile)
            return carry

        lax.fori_loop(0, wc // tile, body, 0)

    def a_copy(c, side, which):
        cols = pl.ds(c * wc, wc)
        quarter_id = ((x_id, far), (y_id, far))[side][which]
        return remote(
            tdx.at[:, quarter_id, pl.ds(side * half, half), cols],
            (ax, ay)[side].at[which, :, :, cols],
            a_ss.at[c, side, which],
            a_rs.at[c, side, which],
            at_exp((x_id, y_id)[side]),
        )

    def b_copy(c, side):
        cols = pl.ds(c * wc, wc)
        return remote(
            bsend.at[side, :, :, cols],
            brecv.at[side, :, :, cols],
            b_ss.at[c, side],
            b_rs.at[c, side],
            at_exp((y_id, x_id)[side]),
        )

    def c_copy(c, p):
        cols = pl.ds(c * wc, wc)
        return remote(
            csend.at[p, :, cols],
            crecv.at[d, :, cols],
            c_ss.at[c, p - 1],
            c_rs.at[c, d],
            (blocks[p], e, t),
        )

    def c_arrival(c, p):
        cols = pl.ds(c * wc, wc)
        return remote(
            csend.at[p, :, cols],
            crecv.at[blocks[p], :, cols],
            c_ss.at[c, p - 1],
            c_rs.at[c, blocks[p]],
            (blocks[p], e, t),
        )

    def start_a(c):
        for which in (1, 0):
            for side in range(2):
                a_copy(c, side, which).start()

    def relay_b(c):
        cols = pl.ds(c * wc, wc)
        for side in range(2):
            a_copy(c, side, 1).wait()
            mine = tdx[:, (y_id, x_id)[side], pl.ds(side * half, half), cols].astype(F32)
            got = (ax, ay)[side][1, :, :, cols].astype(F32)
            bsend[side, :, :, cols] = (mine + got).astype(BF16)
            b_copy(c, side).start()

    def cross_c(c):
        cols = pl.ds(c * wc, wc)
        for side in range(2):
            a_copy(c, side, 0).wait()
            b_copy(c, side).wait()
            part = pl.ds(side * half, half)
            total = tdx[:, e, part, cols].astype(F32)
            total = total + (ax, ay)[side][0, :, :, cols].astype(F32)
            total = total + brecv[side, :, :, cols].astype(F32)
            csend[:, part, cols] = total.astype(BF16)
        for p in range(1, n_dp):
            c_copy(c, p).start()

    def finish(c):
        cols = pl.ds(c * wc, wc)
        total = csend[0, :, cols].astype(F32)
        for p in range(1, n_dp):
            c_copy(c, p).wait_send()
            c_arrival(c, p).wait_recv()
        for p in range(1, n_dp):
            total = total + crecv[blocks[p], :, cols].astype(F32)
        csend[0, :, cols] = (acc[:, cols] + total).astype(BF16)

    dg_rows = hidden_w // dg_chunks
    dg_store = [
        load(dw.at[pl.ds(i * dg_rows, dg_rows)], dg_out.at[pl.ds(i * dg_rows, dg_rows)], dg_sem.at[i])
        for i in range(dg_chunks)
    ]

    def down_grad(i):
        lhs = own[0, :, pl.ds(i * dg_rows, dg_rows)].astype(F32).T.astype(BF16)

        def body(k, carry):
            cols = pl.ds(pl.multiple_of(k * lanes, LANES), lanes)
            dw[pl.ds(i * dg_rows, dg_rows), cols] = dot_nn(lhs, sg[:, cols]).astype(BF16)
            return carry

        lax.fori_loop(0, width // lanes, body, 0)
        dg_store[i].start()

    small = {0: [router_zero], 1: [scale_grads], 3: [router_one], w_chunks: [router_two]}
    fill = [functools.partial(down_grad, i) for i in range(dg_chunks)]

    for c in range(w_chunks + 2):
        if c < w_chunks:
            dx_chunk(c)
            start_a(c)
        elif fill:
            fill.pop(0)()
        for job in small.pop(c, []):
            job()
        if 0 <= c - 2 < w_chunks:
            relay_b(c - 2)
        if 0 <= c - 4 < w_chunks:
            cross_c(c - 4)
    for jobs in small.values():
        for job in jobs:
            job()
    if fill:
        fill.pop(0)()
    for c in range(max(w_chunks - 2, 0), w_chunks):
        cross_c(c)
    router_three()
    for job in fill:
        job()
    rg_store = load(rgt, rg_out, out_sem.at[6])
    rg_store.start()
    for c in range(w_chunks):
        finish(c)

    dx_store = load(csend.at[0], dx_out, out_sem.at[5])
    dx_store.start()
    st_store.wait()
    for copy in own_store:
        copy.wait()
    for copy in dg_store:
        copy.wait()
    dx_store.wait()
    rg_store.wait()


def run_kernel(
    n_dp, n_exp, n_ten, tokens, out_grad, router, chosen, place, gate_w, up_w, down_w
):
    rows, width = tokens.shape
    hidden_w = gate_w.shape[1]
    quarter = rows // n_exp
    half = quarter // 2
    slots = n_dp * CAP
    f_chunks = split_count(hidden_w, 4)
    w_chunks = split_count(width, 6)
    splits = split_count(width - spare_columns(width), 2)
    pieces = splits + 1
    dg_chunks = split_count(hidden_w, 4)
    n_choice = router.shape[0]
    shape = jax.ShapeDtypeStruct
    any_spec = pl.BlockSpec(memory_space=pl.ANY)
    dma = pltpu.SemaphoreType.DMA
    vmem = pltpu.VMEM
    z = n_dp - 1
    m = max(n_ten - 1, 1)
    scratch = [
        vmem((width, hidden_w), BF16),
        vmem((width, hidden_w), BF16),
        vmem((hidden_w, width), BF16),
        vmem((n_dp, n_exp, quarter, width), BF16),
        vmem((n_dp, n_exp, quarter, width), BF16),
        vmem((slots, width), BF16),
        vmem((slots, width), BF16),
        vmem((3, slots, hidden_w), BF16),
        vmem((m, 3, slots, hidden_w), BF16),
        vmem((2, n_dp, half, width), BF16),
        vmem((2, n_dp, half, width), BF16),
        vmem((2, n_dp, half, width), BF16),
        vmem((2, n_dp, half, width), BF16),
        vmem((n_dp, quarter, width), BF16),
        vmem((n_dp, quarter, width), BF16),
        vmem((quarter, width), F32),
        vmem((n_dp, 2, rows), jnp.int32),
        vmem((n_dp, 2, rows), jnp.int32),
        vmem((n_choice, width), BF16),
        vmem((n_dp, n_choice, rows), F32),
        vmem((m, n_dp, n_choice, rows), F32),
        vmem((n_dp, 2, rows), F32),
        vmem((n_dp, LANES, rows), BF16),
        vmem((n_dp, rows, LANES), BF16),
        vmem((slots, LANES), F32),
        vmem((slots, LANES), F32),
        vmem((n_dp, 2, rows), F32),
        vmem((z, n_dp, 2, rows), F32),
        vmem((n_dp, 2, rows), F32),
        vmem((n_dp, 2, rows), F32),
        vmem((n_dp, 2, rows), F32),
        vmem((n_dp, 2, rows), F32),
        vmem((n_dp, 3 * n_choice, rows), F32),
        vmem((rows, rows), F32),
        vmem((n_choice, width), F32),
        dma((6,)),
        dma((2,)),
        dma((2, z)), dma((2, n_dp)),
        dma((2, pieces, n_dp, 2)), dma((2, pieces, n_dp)),
        dma((2, z, splits, 2)), dma((2, z, splits, 2)),
        dma((2, z, splits, 2)), dma((2, z, splits, 2)),
        dma((m, 3, f_chunks)), dma((m, 3, f_chunks)),
        dma((m,)), dma((m,)),
        dma((w_chunks, 2, 2)), dma((w_chunks, 2, 2)),
        dma((w_chunks, 2)), dma((w_chunks, 2)),
        dma((w_chunks, z)), dma((w_chunks, n_dp)),
        dma((z,)), dma((z,)),
        dma((2,)), dma((2,)),
        dma((7,)),
        dma((dg_chunks,)),
    ]
    flops = 2 * slots * width * hidden_w * 5
    return pl.pallas_call(
        functools.partial(layer_kernel, n_dp, n_exp, n_ten, f_chunks, w_chunks, splits, dg_chunks),
        out_shape=(
            shape((slots, hidden_w), BF16),
            shape((slots, hidden_w), BF16),
            shape((slots, width), BF16),
            shape((hidden_w, width), BF16),
            shape((quarter, width), BF16),
            shape((n_choice, width), F32),
        ),
        in_specs=[any_spec] * 8,
        out_specs=(any_spec,) * 6,
        scratch_shapes=scratch,
        compiler_params=pltpu.CompilerParams(
            collective_id=0, has_side_effects=True, vmem_limit_bytes=VMEM_LIMIT
        ),
        cost_estimate=pl.CostEstimate(
            flops=flops, bytes_accessed=6 * width * hidden_w, transcendentals=0
        ),
        name="layer",
    )(
        tokens.reshape(n_exp, quarter, width),
        out_grad.reshape(n_exp, quarter, width),
        router, chosen, place, gate_w, up_w, down_w,
    )


def weight_grads(slot_tokens, grad_gate, grad_up, down):
    slots, width = slot_tokens.shape
    hidden_w = grad_gate.shape[1]
    steps = max(s for s in range(1, 9) if width % (s * LANES) == 0 and hidden_w % (16 * s) == 0)
    tile = width // steps

    def body(st, gg, gu, down_in, gate_out, up_out, down_out):
        lhs = st[...]
        gate_out[...] = dot_tn(lhs, gg[...]).astype(BF16)
        up_out[...] = dot_tn(lhs, gu[...]).astype(BF16)
        down_out[...] = down_in[...]

    whole = pl.BlockSpec((slots, hidden_w), lambda i: (0, 0))
    by_rows = pl.BlockSpec((tile, hidden_w), lambda i: (i, 0))
    down_rows = pl.BlockSpec((hidden_w // steps, width), lambda i: (i, 0))
    shape = jax.ShapeDtypeStruct((width, hidden_w), BF16)
    return pl.pallas_call(
        body,
        grid=(steps,),
        out_shape=(shape, shape, jax.ShapeDtypeStruct((hidden_w, width), BF16)),
        in_specs=[pl.BlockSpec((slots, tile), lambda i: (0, i)), whole, whole, down_rows],
        out_specs=(by_rows, by_rows, down_rows),
        compiler_params=pltpu.CompilerParams(
            dimension_semantics=("arbitrary",), vmem_limit_bytes=VMEM_LIMIT - 2**20
        ),
        cost_estimate=pl.CostEstimate(
            flops=4 * slots * width * hidden_w, bytes_accessed=8 * width * hidden_w, transcendentals=0
        ),
        name="weight_grads",
    )(slot_tokens, grad_gate, grad_up, down)


def build(n_dp, n_exp, n_ten):
    def shards(
        tokens, out_grad, router_weight, gate_weight, up_weight, down_weight, expert_index, slot_index
    ):
        grad_gate, grad_up, slot_tokens, down, tokens_grad, router_t = run_kernel(
            n_dp, n_exp, n_ten, tokens, out_grad, router_weight.T, expert_index.T, slot_index.T,
            gate_weight[0], up_weight[0], down_weight[0],
        )
        gate_grad, up_grad, down_grad = weight_grads(slot_tokens, grad_gate, grad_up, down)
        router_grad = router_t.T
        return (tokens_grad, router_grad, gate_grad[None], up_grad[None], down_grad[None])

    return shards


def solution(mesh):
    in_specs = (
        P("dp", "tensor"),
        P("dp", "tensor"),
        P("tensor", None),
        P("expert", "tensor", "dp"),
        P("expert", "tensor", "dp"),
        P("expert", "dp", "tensor"),
        P("dp", None),
        P("dp", None),
    )
    out_specs = (
        P(("dp", "expert"), "tensor"),
        P("tensor", None),
        P("expert", "tensor", "dp"),
        P("expert", "tensor", "dp"),
        P("expert", "dp", "tensor"),
    )
    shards = build(mesh.shape["dp"], mesh.shape["expert"], mesh.shape["tensor"])
    return jax.shard_map(shards, mesh=mesh, in_specs=in_specs, out_specs=out_specs, check_vma=False)
```

```python
import functools

import jax
import jax.numpy as jnp
from jax import lax
from jax.experimental import pallas as pl
from jax.experimental.pallas import tpu as pltpu
from jax.sharding import PartitionSpec as P

CAP = 96
LAGS = (1, 2)
OWN_AFTER = 1
LEADS = (0.5, 1.5)
EARLY_EVENTS = 3
F32 = jnp.float32
BF16 = jnp.bfloat16
LANES = 128
MESH = pl.DeviceIdType.MESH
VMEM_LIMIT = 67_043_328


def dot_nn(a, b):
    return lax.dot_general(a, b, (((1,), (0,)), ((), ())), preferred_element_type=F32)


def dot_nt(a, b):
    return lax.dot_general(a, b, (((1,), (1,)), ((), ())), preferred_element_type=F32)


def dot_tn(a, b):
    return lax.dot_general(a, b, (((0,), (0,)), ((), ())), preferred_element_type=F32)


def sigmoid(x):
    return 1.0 / (1.0 + jnp.exp(-x))


def three_pieces(x):
    high = x.astype(BF16).astype(F32)
    rest = x - high
    middle = rest.astype(BF16).astype(F32)
    return high, middle, rest - middle


def split_count(width, most):
    for count in range(most, 0, -1):
        if width % (count * LANES) == 0:
            return count
    return 1


def column_chunks(width):
    if width % (12 * LANES) == 0:
        sizes = [width // 12] + [width // 6] * 5 + [width // 12]
    else:
        sizes = [width // split_count(width, 6)] * split_count(width, 6)
    return [(sum(sizes[:i]), sizes[i]) for i in range(len(sizes))]


def spare_columns(width):
    return width // 12 if width % (12 * LANES) == 0 else 0


def layer_kernel(
    n_dp, n_exp, n_ten, f_chunks, splits, dg_chunks,
    tokens, out_grad, router, chosen_in, place_in, gate_w, up_w, down_w,
    gg_out, gu_out, st_out, dg_out, dx_out, rg_out,
    gw, uw, dw, tok, gra, st, sg, own, peer, ax, ay, bsend, brecv, csend, crecv, acc,
    pick, place, rw, logit_own, logit_peer, prob, sel, selt, spb, dacc,
    dsend, dz, d1, dx1, d2, dx2, lgr, term, rgt,
    load_sem, in_sem, idx_ss, idx_rs, z_ss, z_rs, p_ss, p_rs, r_ss, r_rs,
    t_ss, t_rs, lg_ss, lg_rs, a_ss, a_rs, b_ss, b_rs, c_ss, c_rs, dz_ss, dz_rs, de_ss, de_rs, out_sem, dg_sem,
):
    d = lax.axis_index("dp")
    e = lax.axis_index("expert")
    t = lax.axis_index("tensor")
    quarter, width = tok.shape[2], tok.shape[3]
    rows = n_exp * quarter
    half = quarter // 2
    n_choice = rw.shape[0]
    hidden_w = gw.shape[1]
    fc = hidden_w // f_chunks
    chunks = column_chunks(width)
    w_chunks = len(chunks)
    extra = spare_columns(width)
    piece = (width - extra) // splits
    n_pieces = splits + (1 if extra else 0)
    x_id, y_id, far = e ^ 1, e ^ 2, e ^ 3
    tdx = gra
    last = n_dp - 1
    f_tile = fc // split_count(fc, 2)

    def at_dp(k):
        return (lax.rem(d + k, n_dp), e, t)

    def at_exp(which):
        return (d, which, t)

    def at_ten(k):
        return (d, e, lax.rem(t + k, n_ten))

    def remote(src, dst, ss, rs, device):
        return pltpu.make_async_remote_copy(
            src_ref=src, dst_ref=dst, send_sem=ss, recv_sem=rs, device_id=device, device_id_type=MESH
        )

    short = jnp.minimum(d, last - d)
    blocks, from_left = [d], [None]
    for j in range(last):
        inner = j < 2 * short
        distance = jnp.where(inner, j // 2 + 1, j - short + 1)
        left = jnp.where(inner, 1 - j % 2, jnp.where(2 * d > last, 1, 0))
        blocks.append(d + distance * (1 - 2 * left))
        from_left.append(left)
    shifts = range(1, n_dp)

    ins = (tokens, out_grad)
    bufs = (tok, gra)
    slots = (st, sg)
    load = pltpu.make_async_copy
    idx_load = [
        load(chosen_in, pick.at[d], load_sem.at[0]),
        load(place_in, place.at[d], load_sem.at[1]),
    ]
    rw_load = load(router, rw, load_sem.at[2])
    gw_load = load(gate_w, gw, load_sem.at[3])
    uw_load = load(up_w, uw, load_sem.at[4])
    dw_load = load(down_w, dw, load_sem.at[5])
    in_load = [load(ins[a], bufs[a].at[d], in_sem.at[a]) for a in range(2)]
    for copy in idx_load:
        copy.start()
    in_load[0].start()
    rw_load.start()

    barrier = pltpu.get_barrier_semaphore()
    others = [at_dp(k) for k in shifts] + [at_exp(x_id), at_exp(y_id)]
    others += [at_ten(k) for k in range(1, n_ten)]
    for device in others:
        pl.semaphore_signal(barrier, inc=1, device_id=device, device_id_type=MESH)
    pl.semaphore_wait(barrier, len(others))

    def idx_copy(k, which):
        ref = (pick, place)[which].at[d]
        return remote(ref, ref, idx_ss.at[which, k - 1], idx_rs.at[which, d], at_dp(k))

    def idx_arrival(p, which):
        ref = (pick, place)[which].at[blocks[p]]
        return remote(ref, ref, idx_ss.at[which, 0], idx_rs.at[which, blocks[p]], at_dp(1))

    def line_part(ref, h):
        if h == splits:
            return ref.at[:, :, pl.ds(splits * piece, extra)]
        return ref.at[e, :, pl.ds(h * piece, piece)]

    def z_own(a, h, side):
        other = jnp.minimum(d + 1, last) if side == 0 else jnp.maximum(d - 1, 0)
        return remote(
            line_part(ins[a], h),
            line_part(bufs[a].at[d], h),
            z_ss.at[a, h, 0, side],
            z_rs.at[a, h, d],
            (other, e, t),
        )

    def z_hand(a, p, h):
        ref = line_part(bufs[a].at[blocks[p]], h)
        other = jnp.where(from_left[p] == 1, jnp.minimum(d + 1, last), jnp.maximum(d - 1, 0))
        return remote(ref, ref, z_ss.at[a, h, p, 0], z_rs.at[a, h, blocks[p]], (other, e, t))

    def z_goes_on(p):
        return jnp.where(from_left[p] == 1, d < last, d > 0)

    side_open = (d < last, d > 0)

    def send_own(a, h):
        for side in range(2):
            copy = z_own(a, h, side)

            @pl.when(side_open[side])
            def _(copy=copy):
                copy.start()

    def plane_copy(a, p, h, side, quarter_id):
        ref = bufs[a].at[blocks[p], quarter_id, :, pl.ds(h * piece, piece)]
        return remote(
            ref, ref, p_ss.at[a, p - 1, h, side], p_rs.at[a, p - 1, h, side],
            at_exp((x_id, y_id)[side]),
        )

    def relay_copy(a, p, h, side, quarter_id):
        ref = bufs[a].at[
            blocks[p], quarter_id, pl.ds((1 - side) * half, half), pl.ds(h * piece, piece)
        ]
        return remote(
            ref, ref, r_ss.at[a, p - 1, h, side], r_rs.at[a, p - 1, h, side],
            at_exp((x_id, y_id)[side]),
        )

    for h in range(splits):
        send_own(0, h)
    for copy in idx_load:
        copy.wait()
    for k in shifts:
        for which in range(2):
            idx_copy(k, which).start()
    in_load[1].start()
    gw_load.start()
    uw_load.start()
    dw_load.start()

    def hop_line(a, p, h):
        hand = z_hand(a, p, h)
        hand.wait_recv()

        @pl.when(z_goes_on(p))
        def _():
            hand.start()

    def hop_plane(a, p, h):
        plane_copy(a, p, h, 0, e).start()
        plane_copy(a, p, h, 1, e).start()

    def hop_relay(a, p, h):
        plane_copy(a, p, h, 0, x_id).wait_recv()
        relay_copy(a, p, h, 1, x_id).start()
        plane_copy(a, p, h, 1, y_id).wait_recv()
        relay_copy(a, p, h, 0, y_id).start()

    def hop_last(a, p, h):
        relay_copy(a, p, h, 0, far).wait_recv()
        relay_copy(a, p, h, 1, far).wait_recv()

    def to_slots(a, p):
        lanes = width // split_count(width, 6)

        def body(i, carry):
            cols = pl.ds(pl.multiple_of(i * lanes, LANES), lanes)
            values = bufs[a][blocks[p], :, :, cols].reshape(rows, lanes)
            slots[a][pl.ds(p * CAP, CAP), cols] = dot_nn(sel[p, :CAP], values).astype(BF16)
            return carry

        lax.fori_loop(0, width // lanes, body, 0)

    def hits(p, k, count):
        pos = lax.broadcasted_iota(jnp.int32, (count, rows), 0)
        b = blocks[p]
        return (pick[b, k : k + 1] == e) & (place[b, k : k + 1] == pos)

    def make_select(p):
        hot = jnp.where(hits(p, 0, LANES) | hits(p, 1, LANES), 1.0, 0.0).astype(F32)
        sel[p] = hot.astype(BF16)
        selt[p] = hot.T.astype(BF16)

    def part_copy(which, j, k):
        cols = pl.ds(j * fc, fc)
        return remote(
            own.at[which, :, cols],
            peer.at[k - 1, which, :, cols],
            t_ss.at[k - 1, which, j],
            t_rs.at[k - 1, which, j],
            at_ten(k),
        )

    def part_tile(which, j, i):
        sub = pl.ds(pl.multiple_of(j * fc + i * f_tile, LANES), f_tile)
        if which < 2:
            value = dot_nn(st[...], (gw, uw)[which][:, sub])
        else:
            value = dot_nt(sg[...], dw[sub])
        own[which, :, sub] = value.astype(BF16)

    def send_part(which, j):
        for k in range(1, n_ten):
            part_copy(which, j, k).start()

    def part_matmul(which, j):
        def body(i, carry):
            part_tile(which, j, i)
            return carry

        lax.fori_loop(0, fc // f_tile, body, 0)
        send_part(which, j)

    def logits_of(p):
        logit_own[p] = dot_nt(rw[...], tok[blocks[p]].reshape(rows, width))

    def logit_copy(k):
        return remote(
            logit_own, logit_peer.at[k - 1], lg_ss.at[k - 1], lg_rs.at[k - 1], at_ten(k)
        )

    choice = lax.broadcasted_iota(jnp.int32, (n_choice, rows), 0)

    def routing():
        for m in range(1, n_ten):
            logit_copy(m).wait()
        for p in range(n_dp):
            logits = logit_own[p]
            for m in range(1, n_ten):
                logits = logits + logit_peer[m - 1, p]
            b = blocks[p]
            chosen = [
                jnp.sum(jnp.where(choice == pick[b, k : k + 1], logits, 0.0), axis=0, keepdims=True)
                for k in range(2)
            ]
            p0 = sigmoid(chosen[0] - chosen[1])
            p1 = sigmoid(chosen[1] - chosen[0])
            prob[p, 0:1] = p0
            prob[p, 1:2] = p1
            low0 = p0.astype(BF16).astype(F32)
            low1 = p1.astype(BF16).astype(F32)
            picked = jnp.where(hits(p, 0, CAP), low0, 0.0) + jnp.where(hits(p, 1, CAP), low1, 0.0)
            column = jnp.sum(picked, axis=1, keepdims=True)
            spb[pl.ds(p * CAP, CAP)] = jnp.broadcast_to(column, (CAP, LANES))
        dacc[...] = jnp.zeros_like(dacc)

    def mix_block(p, cols):
        base = pl.ds(p * CAP, CAP)
        total = []
        for which in range(3):
            value = own[which, base, cols].astype(F32)
            for k in range(1, n_ten):
                value = value + peer[k - 1, which, base, cols].astype(F32)
            total.append(value)
        g, u, ga = total
        s = sigmoid(g)
        gs = g * s
        hid = (gs * u).astype(BF16)
        dacc[base] = dacc[base] + hid.astype(F32) * ga
        act = spb[base] * ga
        own[0, base, cols] = hid
        own[1, base, cols] = (act * u * s * (1.0 + g * (1.0 - s))).astype(BF16)
        own[2, base, cols] = (act * gs).astype(BF16)

    def mix_wait(j):
        for which in range(3):
            for k in range(1, n_ten):
                part_copy(which, j, k).wait()

    def mix_tile(j, i):
        for q in range(f_tile // LANES):
            cols = pl.ds(pl.multiple_of(j * fc + i * f_tile + q * LANES, LANES), LANES)
            for p in range(n_dp):
                mix_block(p, cols)

    def mix(j):
        mix_wait(j)

        def body(i, carry):
            mix_tile(j, i)
            return carry

        lax.fori_loop(0, fc // f_tile, body, 0)

    pairs = [range(p, min(p + 2, n_dp)) for p in range(1, n_dp, 2)]
    orders = [[(a, p, h) for pair in pairs for h in range(splits) for p in pair] for a in range(2)]
    order = orders[0] + orders[1]
    beyond = [[(a, p, splits) for p in range(1, n_dp)] if extra else [] for a in range(2)]
    events = []
    for i, (a, p, h) in enumerate(order):
        lag = LAGS[a]
        ahead = LEADS[a] if i else 0
        events.append((i - ahead, 0, hop_line, (a, p, h)))
        events.append((i, 1, hop_plane, (a, p, h)))
        events.append((i + lag, 2, hop_relay, (a, p, h)))
        events.append((i + 2 * lag, 3, hop_last, (a, p, h)))
    for a in range(2):
        for i, which in enumerate(beyond[a]):
            time = len(orders[0]) * (a + 1) - len(beyond[a]) + i
            events.append((time + 0.5, 4, hop_line, which))
    events.sort(key=lambda event: event[:2])
    work = []
    left = [set(orders[a] + beyond[a]) for a in range(2)]
    events_left = len(events)
    tokens_done = False
    for position, (_, _, hop, which) in enumerate(events):
        hop(*which)
        events_left -= 1
        if position == EARLY_EVENTS:
            make_select(0)
            rw_load.wait()
            in_load[0].wait()
            to_slots(0, 0)
            logits_of(0)
        if hop is hop_line:
            if which == order[len(pairs[0]) - 1]:
                for h in range(splits, n_pieces):
                    send_own(0, h)
            if which == orders[0][OWN_AFTER]:
                for h in range(n_pieces):
                    send_own(1, h)
        if hop is hop_last or which[2] == splits:
            a, p, h = which
            left[a].discard(which)
            if not any(other[1] == p for other in left[a]):
                if a == 0:
                    for kind in range(2):
                        idx_arrival(p, kind).wait_recv()
                    make_select(p)
                    logits_of(p)
                to_slots(a, p)
            if a == 0 and not left[0]:
                for m in range(1, n_ten):
                    logit_copy(m).start()
                in_load[1].wait()
                to_slots(1, 0)
                gw_load.wait()
                uw_load.wait()
                work += [functools.partial(part_matmul, w, j) for w in range(2) for j in range(f_chunks)]
                work.append(routing)
                tokens_done = True
        if tokens_done and work and hop in (hop_plane, hop_relay, hop_last):
            work.pop(0)()
    for job in work:
        job()
    dw_load.wait()

    for k in shifts:
        for which in range(2):
            idx_copy(k, which).wait_send()
    for a in range(2):
        for h in range(n_pieces):
            for side in range(2):
                copy = z_own(a, h, side)

                @pl.when(side_open[side])
                def _(copy=copy):
                    copy.wait_send()

    for a, p, h in order + beyond[0] + beyond[1]:
        hand = z_hand(a, p, h)

        @pl.when(z_goes_on(p))
        def _(hand=hand):
            hand.wait_send()

    for a, p, h in order:
        for side in range(2):
            plane_copy(a, p, h, side, e).wait_send()
            relay_copy(a, p, h, 1 - side, (x_id, y_id)[side]).wait_send()
    for j in range(f_chunks + 1):
        if j < f_chunks:
            part_matmul(2, j)
        if j >= 1:
            mix(j - 1)

    st_store = load(st, st_out, out_sem.at[3])
    st_store.start()
    own_store = [
        load(own.at[w], (None, gg_out, gu_out)[w], out_sem.at[w]) for w in (1, 2)
    ]
    for copy in own_store:
        copy.start()

    def router_zero():
        for p in range(n_dp):
            column = jnp.sum(dacc[pl.ds(p * CAP, CAP)], axis=1, keepdims=True)
            for k in range(2):
                dsend[blocks[p], k : k + 1] = jnp.sum(
                    jnp.where(hits(p, k, CAP), column, 0.0), axis=0, keepdims=True
                )
        for k in shifts:
            dz_copy(k).start()

    def dz_copy(k):
        return remote(dsend, dz.at[k - 1], dz_ss.at[k - 1], dz_rs.at[k - 1], at_dp(k))

    def de_copy(side):
        return remote(
            (d1, d2)[side], (dx1, dx2)[side], de_ss.at[side], de_rs.at[side],
            at_exp((x_id, y_id)[side]),
        )

    def scale_grads():
        lanes = width // split_count(width, 6)

        def body(i, carry):
            cols = pl.ds(pl.multiple_of(i * lanes, LANES), lanes)
            for p in range(n_dp):
                base = pl.ds(p * CAP, CAP)
                sg[base, cols] = (spb[base][:, 0:1] * sg[base, cols].astype(F32)).astype(BF16)
            return carry

        lax.fori_loop(0, width // lanes, body, 0)

    def router_one():
        total = dsend[...]
        for k in shifts:
            dz_copy(k).wait()
        for k in shifts:
            total = total + dz[k - 1]
        d1[...] = total
        de_copy(0).start()

    def router_two():
        de_copy(0).wait()
        d2[...] = d1[...] + dx1[...]
        de_copy(1).start()

    lanes = width // split_count(width, 6)

    def router_three():
        de_copy(1).wait()
        dx2[...] = d2[...] + dx2[...]
        for p in range(n_dp):
            b = blocks[p]
            g0, g1 = dx2[b, 0:1], dx2[b, 1:2]
            p0, p1 = prob[p, 0:1], prob[p, 1:2]
            mixed = p0 * g0 + p1 * g1
            w0, w1 = p0 * (g0 - mixed), p1 * (g1 - mixed)
            lg = jnp.where(choice == pick[b, 0:1], w0, 0.0) + jnp.where(
                choice == pick[b, 1:2], w1, 0.0
            )
            for i, part in enumerate(three_pieces(lg)):
                lgr[p, pl.ds(n_choice * i, n_choice)] = part
        weights = jnp.concatenate([rw[...].astype(F32)] * 3, axis=0).astype(BF16)

        def body(i, carry):
            cols = pl.ds(pl.multiple_of(i * lanes, LANES), lanes)
            out = jnp.zeros((3 * n_choice, lanes), F32)
            for p in range(n_dp):
                values = tok[blocks[p], :, :, cols].reshape(rows, lanes)
                out = out + dot_nn(lgr[p].astype(BF16), values)
            rgt[:, cols] = (
                out[0:n_choice] + out[n_choice : 2 * n_choice] + out[2 * n_choice : 3 * n_choice]
            )
            return carry

        lax.fori_loop(0, width // lanes, body, 0)
        term[...] = jnp.zeros_like(term)
        term[pl.ds(0, 3 * n_choice)] = lgr[0]
        term[...] = term[...].T
        mine = term[pl.ds(pl.multiple_of(e * quarter, 8), quarter)][:, : 3 * n_choice].astype(BF16)
        for i in range(width // lanes):
            cols = slice(i * lanes, (i + 1) * lanes)
            acc[:, cols] = dot_nn(mine, weights[:, cols])

    def dx_chunk(c):
        first, size = chunks[c]
        tile = min(size, 2 * LANES)

        def body(i, carry):
            cols = pl.ds(pl.multiple_of(first + i * tile, LANES), tile)
            part = dot_nt(own[1], gw[cols]) + dot_nt(own[2], uw[cols])
            part = part.astype(BF16)
            for p in range(n_dp):
                one = dot_nn(selt[p][:, :CAP], part[p * CAP : (p + 1) * CAP]).astype(BF16)
                tdx[p, :, :, cols] = one.reshape(n_exp, quarter, tile)
            return carry

        lax.fori_loop(0, size // tile, body, 0)

    def a_copy(c, side, which):
        cols = pl.ds(*chunks[c])
        quarter_id = ((x_id, far), (y_id, far))[side][which]
        return remote(
            tdx.at[:, quarter_id, pl.ds(side * half, half), cols],
            (ax, ay)[side].at[which, :, :, cols],
            a_ss.at[c, side, which],
            a_rs.at[c, side, which],
            at_exp((x_id, y_id)[side]),
        )

    def b_copy(c, side):
        cols = pl.ds(*chunks[c])
        return remote(
            bsend.at[side, :, :, cols],
            brecv.at[side, :, :, cols],
            b_ss.at[c, side],
            b_rs.at[c, side],
            at_exp((y_id, x_id)[side]),
        )

    def c_copy(c, p):
        cols = pl.ds(*chunks[c])
        return remote(
            csend.at[p, :, cols],
            crecv.at[d, :, cols],
            c_ss.at[c, p - 1],
            c_rs.at[c, d],
            (blocks[p], e, t),
        )

    def c_arrival(c, p):
        cols = pl.ds(*chunks[c])
        return remote(
            csend.at[p, :, cols],
            crecv.at[blocks[p], :, cols],
            c_ss.at[c, p - 1],
            c_rs.at[c, blocks[p]],
            (blocks[p], e, t),
        )

    def start_a(c):
        for which in (1, 0):
            for side in range(2):
                a_copy(c, side, which).start()

    def relay_b(c):
        cols = pl.ds(*chunks[c])
        for side in range(2):
            a_copy(c, side, 1).wait()
            mine = tdx[:, (y_id, x_id)[side], pl.ds(side * half, half), cols].astype(F32)
            got = (ax, ay)[side][1, :, :, cols].astype(F32)
            bsend[side, :, :, cols] = (mine + got).astype(BF16)
            b_copy(c, side).start()

    def cross_c(c):
        cols = pl.ds(*chunks[c])
        for side in range(2):
            a_copy(c, side, 0).wait()
            b_copy(c, side).wait()
            part = pl.ds(side * half, half)
            total = tdx[:, e, part, cols].astype(F32)
            total = total + (ax, ay)[side][0, :, :, cols].astype(F32)
            total = total + brecv[side, :, :, cols].astype(F32)
            csend[:, part, cols] = total.astype(BF16)
        for p in range(1, n_dp):
            c_copy(c, p).start()

    def finish(c):
        cols = pl.ds(*chunks[c])
        total = csend[0, :, cols].astype(F32)
        for p in range(1, n_dp):
            c_copy(c, p).wait_send()
            c_arrival(c, p).wait_recv()
        for p in range(1, n_dp):
            total = total + crecv[blocks[p], :, cols].astype(F32)
        csend[0, :, cols] = (acc[:, cols] + total).astype(BF16)

    dg_rows = hidden_w // dg_chunks
    dg_store = [
        load(dw.at[pl.ds(i * dg_rows, dg_rows)], dg_out.at[pl.ds(i * dg_rows, dg_rows)], dg_sem.at[i])
        for i in range(dg_chunks)
    ]

    dg_lanes = width // split_count(width, 3)

    def down_grad(i):
        lhs = own[0, :, pl.ds(i * dg_rows, dg_rows)].astype(F32).T.astype(BF16)

        def body(k, carry):
            cols = pl.ds(pl.multiple_of(k * dg_lanes, LANES), dg_lanes)
            dw[pl.ds(i * dg_rows, dg_rows), cols] = dot_nn(lhs, sg[:, cols]).astype(BF16)
            return carry

        lax.fori_loop(0, width // dg_lanes, body, 0)
        dg_store[i].start()

    small = {0: [router_zero], 1: [scale_grads], 3: [router_one], w_chunks: [router_two]}
    fill = [functools.partial(down_grad, i) for i in range(dg_chunks)]

    for c in range(w_chunks + 2):
        if c < w_chunks:
            dx_chunk(c)
            start_a(c)
        elif fill:
            fill.pop(0)()
        for job in small.pop(c, []):
            job()
        if 0 <= c - 2 < w_chunks:
            relay_b(c - 2)
        if 0 <= c - 4 < w_chunks:
            cross_c(c - 4)
    for jobs in small.values():
        for job in jobs:
            job()
    if fill:
        fill.pop(0)()
    for c in range(max(w_chunks - 2, 0), w_chunks):
        cross_c(c)
    router_three()
    for job in fill:
        job()
    rg_store = load(rgt, rg_out, out_sem.at[6])
    rg_store.start()
    for c in range(w_chunks):
        finish(c)

    dx_store = load(csend.at[0], dx_out, out_sem.at[5])
    dx_store.start()
    st_store.wait()
    for copy in own_store:
        copy.wait()
    for copy in dg_store:
        copy.wait()
    dx_store.wait()
    rg_store.wait()


def run_kernel(
    n_dp, n_exp, n_ten, tokens, out_grad, router, chosen, place, gate_w, up_w, down_w
):
    rows, width = tokens.shape
    hidden_w = gate_w.shape[1]
    quarter = rows // n_exp
    half = quarter // 2
    slots = n_dp * CAP
    f_chunks = split_count(hidden_w, 4)
    w_chunks = len(column_chunks(width))
    splits = split_count(width - spare_columns(width), 2)
    pieces = splits + 1
    dg_chunks = split_count(hidden_w, 4)
    n_choice = router.shape[0]
    shape = jax.ShapeDtypeStruct
    any_spec = pl.BlockSpec(memory_space=pl.ANY)
    dma = pltpu.SemaphoreType.DMA
    vmem = pltpu.VMEM
    z = n_dp - 1
    m = max(n_ten - 1, 1)
    scratch = [
        vmem((width, hidden_w), BF16),
        vmem((width, hidden_w), BF16),
        vmem((hidden_w, width), BF16),
        vmem((n_dp, n_exp, quarter, width), BF16),
        vmem((n_dp, n_exp, quarter, width), BF16),
        vmem((slots, width), BF16),
        vmem((slots, width), BF16),
        vmem((3, slots, hidden_w), BF16),
        vmem((m, 3, slots, hidden_w), BF16),
        vmem((2, n_dp, half, width), BF16),
        vmem((2, n_dp, half, width), BF16),
        vmem((2, n_dp, half, width), BF16),
        vmem((2, n_dp, half, width), BF16),
        vmem((n_dp, quarter, width), BF16),
        vmem((n_dp, quarter, width), BF16),
        vmem((quarter, width), F32),
        vmem((n_dp, 2, rows), jnp.int32),
        vmem((n_dp, 2, rows), jnp.int32),
        vmem((n_choice, width), BF16),
        vmem((n_dp, n_choice, rows), F32),
        vmem((m, n_dp, n_choice, rows), F32),
        vmem((n_dp, 2, rows), F32),
        vmem((n_dp, LANES, rows), BF16),
        vmem((n_dp, rows, LANES), BF16),
        vmem((slots, LANES), F32),
        vmem((slots, LANES), F32),
        vmem((n_dp, 2, rows), F32),
        vmem((z, n_dp, 2, rows), F32),
        vmem((n_dp, 2, rows), F32),
        vmem((n_dp, 2, rows), F32),
        vmem((n_dp, 2, rows), F32),
        vmem((n_dp, 2, rows), F32),
        vmem((n_dp, 3 * n_choice, rows), F32),
        vmem((rows, rows), F32),
        vmem((n_choice, width), F32),
        dma((6,)),
        dma((2,)),
        dma((2, z)), dma((2, n_dp)),
        dma((2, pieces, n_dp, 2)), dma((2, pieces, n_dp)),
        dma((2, z, splits, 2)), dma((2, z, splits, 2)),
        dma((2, z, splits, 2)), dma((2, z, splits, 2)),
        dma((m, 3, f_chunks)), dma((m, 3, f_chunks)),
        dma((m,)), dma((m,)),
        dma((w_chunks, 2, 2)), dma((w_chunks, 2, 2)),
        dma((w_chunks, 2)), dma((w_chunks, 2)),
        dma((w_chunks, z)), dma((w_chunks, n_dp)),
        dma((z,)), dma((z,)),
        dma((2,)), dma((2,)),
        dma((7,)),
        dma((dg_chunks,)),
    ]
    flops = 2 * slots * width * hidden_w * 5
    return pl.pallas_call(
        functools.partial(layer_kernel, n_dp, n_exp, n_ten, f_chunks, splits, dg_chunks),
        out_shape=(
            shape((slots, hidden_w), BF16),
            shape((slots, hidden_w), BF16),
            shape((slots, width), BF16),
            shape((hidden_w, width), BF16),
            shape((quarter, width), BF16),
            shape((n_choice, width), F32),
        ),
        in_specs=[any_spec] * 8,
        out_specs=(any_spec,) * 6,
        scratch_shapes=scratch,
        compiler_params=pltpu.CompilerParams(
            collective_id=0, has_side_effects=True, vmem_limit_bytes=VMEM_LIMIT
        ),
        cost_estimate=pl.CostEstimate(
            flops=flops, bytes_accessed=6 * width * hidden_w, transcendentals=0
        ),
        name="layer",
    )(
        tokens.reshape(n_exp, quarter, width),
        out_grad.reshape(n_exp, quarter, width),
        router, chosen, place, gate_w, up_w, down_w,
    )


def weight_grads(slot_tokens, grad_gate, grad_up, down):
    slots, width = slot_tokens.shape
    hidden_w = grad_gate.shape[1]
    steps = max(s for s in range(1, 5) if width % (s * LANES) == 0 and hidden_w % (16 * s) == 0)
    tile = width // steps

    def body(st, gg, gu, down_in, gate_out, up_out, down_out):
        lhs = st[...]
        gate_out[...] = dot_tn(lhs, gg[...]).astype(BF16)
        up_out[...] = dot_tn(lhs, gu[...]).astype(BF16)
        down_out[...] = down_in[...]

    whole = pl.BlockSpec((slots, hidden_w), lambda i: (0, 0))
    by_rows = pl.BlockSpec((tile, hidden_w), lambda i: (i, 0))
    down_rows = pl.BlockSpec((hidden_w // steps, width), lambda i: (i, 0))
    shape = jax.ShapeDtypeStruct((width, hidden_w), BF16)
    return pl.pallas_call(
        body,
        grid=(steps,),
        out_shape=(shape, shape, jax.ShapeDtypeStruct((hidden_w, width), BF16)),
        in_specs=[pl.BlockSpec((slots, tile), lambda i: (0, i)), whole, whole, down_rows],
        out_specs=(by_rows, by_rows, down_rows),
        compiler_params=pltpu.CompilerParams(
            dimension_semantics=("arbitrary",), vmem_limit_bytes=VMEM_LIMIT - 2**20
        ),
        cost_estimate=pl.CostEstimate(
            flops=4 * slots * width * hidden_w, bytes_accessed=8 * width * hidden_w, transcendentals=0
        ),
        name="weight_grads",
    )(slot_tokens, grad_gate, grad_up, down)


def build(n_dp, n_exp, n_ten):
    def shards(
        tokens, out_grad, router_weight, gate_weight, up_weight, down_weight, expert_index, slot_index
    ):
        grad_gate, grad_up, slot_tokens, down, tokens_grad, router_t = run_kernel(
            n_dp, n_exp, n_ten, tokens, out_grad, router_weight.T, expert_index.T, slot_index.T,
            gate_weight[0], up_weight[0], down_weight[0],
        )
        gate_grad, up_grad, down_grad = weight_grads(slot_tokens, grad_gate, grad_up, down)
        router_grad = router_t.T
        return (tokens_grad, router_grad, gate_grad[None], up_grad[None], down_grad[None])

    return shards


def solution(mesh):
    in_specs = (
        P("dp", "tensor"),
        P("dp", "tensor"),
        P("tensor", None),
        P("expert", "tensor", "dp"),
        P("expert", "tensor", "dp"),
        P("expert", "dp", "tensor"),
        P("dp", None),
        P("dp", None),
    )
    out_specs = (
        P(("dp", "expert"), "tensor"),
        P("tensor", None),
        P("expert", "tensor", "dp"),
        P("expert", "tensor", "dp"),
        P("expert", "dp", "tensor"),
    )
    shards = build(mesh.shape["dp"], mesh.shape["expert"], mesh.shape["tensor"])
    return jax.shard_map(shards, mesh=mesh, in_specs=in_specs, out_specs=out_specs, check_vma=False)
```
